32 devices in a mesh: lat: 4 (over z), lon: 8 (over y, x, core).
Axes of the slice: x: 2, y: 2, z: 4, core: 2. Of those that a mesh axis runs over, the one named last changes fastest.
Arguments:
- tokens: bfloat16 [96, 384, 512], P('lat', 'lon'), may hold values from -8 to 8
- lat_band: int32 [96], replicated, may hold values from 0 to 7, as said below
- gain_attn: float32 [512], replicated, may hold values from 0.1 to 1.9
- w_qkv: bfloat16 [512, 1536], replicated, may hold values from -1.5 to 1.5
- w_out: bfloat16 [512, 512], replicated, may hold values from -0.25 to 0.25
- gain_merge: float32 [2048], replicated, may hold values from 0.1 to 1.9
- w_merge: bfloat16 [2048, 1024], replicated, may hold values from -0.125 to 0.125
- grad_merged: bfloat16 [48, 192, 1024], P('lat', 'lon'), may hold values from -6 to 6
Outputs:
- merged: bfloat16 [48, 192, 1024], P('lat', 'lon')
- grad_tokens: float32 [96, 384, 512], P('lat', 'lon')
- grad_gain_attn: float32 [512], replicated
- grad_w_qkv: float32 [512, 1536], replicated
- grad_w_out: float32 [512, 512], replicated
- grad_gain_merge: float32 [2048], replicated
- grad_w_merge: float32 [2048, 1024], replicated
The draws below stay inside these ranges and needn't reach their ends.
Inputs may be any that keep to these rules, and one draw needn't show every extreme that they name: `lat_band`: band number of each latitude row; it never falls from one row to the next, and every band holds at least one row.
All inputs are finite; a program needn't handle non-finite values.
Results may differ from the reference program's by a relative error of at most 0.025.
Values may be sent and summed in bfloat16 or wider, within the bound.
No kernel may reach another device: no remote copies, remote signals or barrier semaphores. Data moves between devices by JAX's collectives and lax.ppermute only.
A program may use at most 192 MiB of HBM per device.

```python
import jax
import jax.numpy as jnp
from jax import lax

C1 = 512
C2 = 1024
HEADS = 8
WLAT = 6
WLON = 12
NLAT = 96
NLON = 384


def draw_lat_band(key, part):
    band_total = max(2, NLAT // 12)
    order = jax.random.permutation(jax.random.fold_in(key, 31), NLAT - 1).astype(jnp.int32) + 1
    cut_rows = order[:band_total - 1]
    row_ids = jnp.arange(NLAT, dtype=jnp.int32)
    above = (row_ids[:, None] >= cut_rows[None, :]).astype(jnp.int32)
    return jnp.sum(above, axis=1).astype(jnp.int32)


def draw_tokens(key, part):
    values = jnp.clip(jax.random.normal(jax.random.fold_in(key, 11), (NLAT, NLON, C1), jnp.float32), -6.0, 6.0)
    return values.astype(jnp.bfloat16)


def draw_w_qkv(key, part):
    scale = C1 ** (-0.5)
    values = jnp.clip(jax.random.normal(jax.random.fold_in(key, 21), (C1, 3 * C1), jnp.float32), -6.0, 6.0) * scale
    return values.astype(jnp.bfloat16)


def level_of(rng, extent, pieces, smallest, top_value):
    factor_of, own = 1.0, jax.random.fold_in(rng, 6)
    for dim, parts in pieces:
        draws = jnp.exp(jax.random.uniform(jax.random.fold_in(own, dim), (parts,), jnp.float32, smallest / len(pieces), top_value / len(pieces)))
        factor_of = factor_of * jnp.repeat(draws, extent[dim] // parts).reshape([-1 if axis == dim else 1 for axis in range(len(extent))])
    return factor_of


def centred(key, dims, scale, most, shards=(), kind=jnp.bfloat16):
    values = scale * jax.random.normal(key, dims, jnp.float32)
    if shards:
        values = values * level_of(key, dims, shards, -0.22, 0.18)
    return jnp.clip(values, -most, most).astype(kind)


def setup_inputs(seed: int = 0) -> dict:
    keys = jax.random.split(jax.random.key(seed), 9)
    tokens = draw_tokens(jax.random.fold_in(keys[8], 71), 0)
    lat_band = draw_lat_band(jax.random.fold_in(keys[8], 71), 0)
    gain_attn = jnp.clip(1.0 + 0.18 * jax.random.normal(keys[2], (C1,), jnp.float32), 0.1, 1.9)
    w_qkv = draw_w_qkv(jax.random.fold_in(keys[8], 71), 0)
    w_out = centred(keys[4], (C1, C1), C1 ** -0.5, 0.25)
    gain_merge = jnp.clip(1.0 + 0.18 * jax.random.normal(keys[5], (4 * C1,), jnp.float32), 0.1, 1.9)
    w_merge = centred(keys[6], (4 * C1, C2), (4 * C1) ** -0.5, 0.125)
    grad_merged = centred(keys[7], (NLAT // 2, NLON // 2, C2), 1.0, 6.0, ((0, 4), (1, 8)))
    return dict(tokens=tokens, lat_band=lat_band, gain_attn=gain_attn, w_qkv=w_qkv, w_out=w_out, gain_merge=gain_merge, w_merge=w_merge, grad_merged=grad_merged)


EPSILON = 1e-05

def normalize(values, gain_vec):
    average = lax.optimization_barrier(jnp.mean(values, axis=-1, keepdims=True))
    centered = values - average
    variance = lax.optimization_barrier(jnp.mean(centered * centered, axis=-1, keepdims=True))
    return centered * lax.rsqrt(variance + EPSILON) * gain_vec

def windows_attend(qkv_grid, band_rows, head_count):
    grid_rows, grid_cols, triple = qkv_grid.shape
    features = triple // 3
    head_size = features // head_count
    count_a = grid_rows // WLAT
    count_b = grid_cols // WLON
    window_size = WLAT * WLON
    blocks = qkv_grid.reshape(count_a, WLAT, count_b, WLON, 3, head_count, head_size)
    blocks = blocks.transpose(4, 0, 2, 5, 1, 3, 6).reshape(3, count_a, count_b, head_count, window_size, head_size)
    queries = blocks[0].astype(jnp.float32)
    key_rows = blocks[1].astype(jnp.float32)
    value_rows = blocks[2].astype(jnp.float32)
    scores = jnp.einsum('abhqd,abhkd->abhqk', queries, key_rows) * head_size ** (-0.5)
    labels = jnp.repeat(band_rows.reshape(count_a, WLAT), WLON, axis=1)
    allowed = labels[:, :, None] == labels[:, None, :]
    scores = jnp.where(allowed[:, None, None, :, :], scores, -1e+30)
    attn_weights = jax.nn.softmax(scores, axis=-1).astype(jnp.bfloat16)
    attn_out = jnp.einsum('abhqk,abhkd->abhqd', attn_weights.astype(jnp.float32), value_rows).astype(jnp.bfloat16)
    attn_out = attn_out.reshape(count_a, count_b, head_count, WLAT, WLON, head_size)
    return attn_out.transpose(0, 3, 1, 4, 2, 5).reshape(grid_rows, grid_cols, features)

def merge_groups(mixed_tokens):
    grid_rows, grid_cols, features = mixed_tokens.shape
    grouped = mixed_tokens.reshape(grid_rows // 2, 2, grid_cols // 2, 2, features).transpose(0, 2, 3, 1, 4)
    return grouped.reshape(grid_rows // 2, grid_cols // 2, 4 * features)

def reference(tokens, lat_band, gain_attn, w_qkv, w_out, gain_merge, w_merge, grad_merged):
    features = tokens.shape[2]
    half_lat = WLAT // 2
    half_lon = WLON // 2
    inputs = tokens.astype(jnp.float32)

    def section_one(values, gain_vec):
        return normalize(values, gain_vec).astype(jnp.bfloat16)
    normed, first_back = jax.vjp(section_one, inputs, gain_attn)
    flat_normed = normed.reshape(-1, features)
    qkv_grid = jnp.dot(flat_normed, w_qkv, preferred_element_type=jnp.float32).astype(jnp.bfloat16)
    qkv_grid = qkv_grid.reshape(NLAT, NLON, 3 * features)
    rolled = jnp.roll(qkv_grid, (-half_lat, -half_lon), (0, 1))
    band_rows = jnp.roll(lat_band, -half_lat)

    def section_two(values):
        return windows_attend(values, band_rows, HEADS)
    attended, second_back = jax.vjp(section_two, rolled)
    attended = jnp.roll(attended, (half_lat, half_lon), (0, 1))
    flat_att = attended.reshape(-1, features)
    projected = jnp.dot(flat_att, w_out, preferred_element_type=jnp.float32).reshape(NLAT, NLON, features)
    mixed_tokens = (inputs + projected).astype(jnp.bfloat16)

    def section_three(values, gain_vec):
        return normalize(merge_groups(values).astype(jnp.float32), gain_vec).astype(jnp.bfloat16)
    merged_in, third_back = jax.vjp(section_three, mixed_tokens, gain_merge)
    flat_in = merged_in.reshape(-1, 4 * features)
    flat_grad = grad_merged.reshape(-1, grad_merged.shape[2])
    merged = jnp.dot(flat_in, w_merge, preferred_element_type=jnp.float32).astype(jnp.bfloat16).reshape(grad_merged.shape)
    grad_w_merge = jnp.dot(flat_in.T, flat_grad, preferred_element_type=jnp.float32)
    grad_in = jnp.dot(flat_grad, w_merge.T, preferred_element_type=jnp.float32).astype(jnp.bfloat16).reshape(merged_in.shape)
    grad_mixed, grad_gain_merge = third_back(grad_in)
    flat_mixed = grad_mixed.reshape(-1, features)
    grad_w_out = jnp.dot(flat_att.T, flat_mixed, preferred_element_type=jnp.float32)
    grad_att = jnp.dot(flat_mixed, w_out.T, preferred_element_type=jnp.float32).astype(jnp.bfloat16)
    grad_att = grad_att.reshape(NLAT, NLON, features)
    grad_rolled, = second_back(jnp.roll(grad_att, (-half_lat, -half_lon), (0, 1)))
    grad_qkv = jnp.roll(grad_rolled, (half_lat, half_lon), (0, 1)).reshape(-1, 3 * features)
    grad_w_qkv = jnp.dot(flat_normed.T, grad_qkv, preferred_element_type=jnp.float32)
    grad_normed = jnp.dot(grad_qkv, w_qkv.T, preferred_element_type=jnp.float32).astype(jnp.bfloat16)
    grad_inputs, grad_gain_attn = first_back(grad_normed.reshape(NLAT, NLON, features))
    grad_tokens = grad_inputs + grad_mixed.astype(jnp.float32)
    return (merged, grad_tokens, grad_gain_attn, grad_w_qkv, grad_w_out, grad_gain_merge, grad_w_merge)
```

```python
import functools

import jax
import jax.numpy as jnp
import numpy as np
from jax import lax
from jax.experimental import pallas as pl
from jax.experimental.pallas import tpu as pltpu
from jax.sharding import PartitionSpec as P

HEADS = 8
WLAT = 6
WLON = 12
EPSILON = 1e-05
BF = jnp.bfloat16
F32 = jnp.float32


def dot_nn(a, b):
    return lax.dot_general(a, b, (((1,), (0,)), ((), ())), preferred_element_type=F32)


def dot_nt(a, b):
    return lax.dot_general(a, b, (((1,), (1,)), ((), ())), preferred_element_type=F32)


def dot_tn(a, b):
    return lax.dot_general(a, b, (((0,), (0,)), ((), ())), preferred_element_type=F32)


def params(steps):
    return pltpu.CompilerParams(
        dimension_semantics=("arbitrary",) * steps, vmem_limit_bytes=60 * 1024 * 1024
    )


def cost(flops, nbytes):
    return pl.CostEstimate(flops=int(flops), transcendentals=0, bytes_accessed=int(nbytes))


def window_matrix(cols, stride):
    count_b = cols // WLON
    mat = np.zeros((count_b * stride, WLAT * cols), np.float32)
    for b in range(count_b):
        for r in range(WLAT):
            for c in range(WLON):
                mat[b * stride + r * WLON + c, r * cols + b * WLON + c] = 1.0
    return mat


def patch_matrix(cols):
    half = cols // 2
    mat = np.zeros((4 * half, 2 * cols), np.float32)
    for j in range(half):
        for g, (dr, dc) in enumerate(((0, 0), (1, 0), (0, 1), (1, 1))):
            mat[g * half + j, dr * cols + 2 * j + dc] = 1.0
    return mat


def lane_masks():
    lane = lax.broadcasted_iota(jnp.int32, (1, 128), 1)
    even = (lane < 64).astype(F32)
    return even.astype(BF), (1.0 - even).astype(BF)


def forward_kernel(stride, count_b, x_ref, allow_ref, gain_ref, w_ref, to_win_ref, to_grid_ref,
                   att_ref, qkv_ref, normed_ref, att_win_ref):
    features = x_ref.shape[1]
    x = dot_nn(to_win_ref[...], x_ref[...])
    average = jnp.mean(x, axis=-1, keepdims=True)
    centered = x - average
    variance = jnp.mean(centered * centered, axis=-1, keepdims=True)
    normed = (centered * lax.rsqrt(variance + EPSILON) * gain_ref[...]).astype(BF)
    normed_ref[...] = normed
    qkv_ref[...] = dot_nn(normed, w_ref[...]).astype(BF)
    allow = allow_ref[0] > 0.5
    masks = lane_masks()
    for b in range(count_b):
        rows = slice(b * stride, (b + 1) * stride)
        for pair in range(features // 128):
            q2 = qkv_ref[rows, pl.ds(128 * pair, 128)] * jnp.asarray(0.125, BF)
            k2 = qkv_ref[rows, pl.ds(features + 128 * pair, 128)]
            v2 = qkv_ref[rows, pl.ds(2 * features + 128 * pair, 128)]
            total = None
            for m in masks:
                s = dot_nt(q2, k2 * m)
                s = jnp.where(allow, s, -1e30)
                s = s - jnp.max(s, axis=-1, keepdims=True)
                e = jnp.exp(s)
                p = (e / jnp.sum(e, axis=-1, keepdims=True)).astype(BF)
                o = dot_nn(p, v2 * m)
                total = o if total is None else total + o
            att_win_ref[rows, pl.ds(128 * pair, 128)] = total.astype(BF)
    att_ref[...] = dot_nn(to_grid_ref[...], att_win_ref[...]).astype(BF)


def middle_kernel(cols, tok_ref, att_ref, w_out_ref, gain_ref, w_merge_ref, gm_ref, to_patch_ref,
                  from_patch_ref, merged_in_ref, grad_mixed_ref, grad_att_ref):
    tokens, features = tok_ref.shape
    pairs = tokens // (2 * cols)
    half = cols // 2
    mixed = (tok_ref[...].astype(F32) + dot_nn(att_ref[...], w_out_ref[...])).astype(BF)
    parts = [dot_nn(to_patch_ref[...], mixed[2 * cols * i : 2 * cols * (i + 1)]) for i in range(pairs)]
    groups = [
        jnp.concatenate([part[half * g : half * (g + 1)] for part in parts], axis=0) for g in range(4)
    ]
    width = 4 * features
    average = sum(jnp.sum(v, axis=-1, keepdims=True) for v in groups) / width
    groups = [v - average for v in groups]
    variance = sum(jnp.sum(v * v, axis=-1, keepdims=True) for v in groups) / width
    inv = lax.rsqrt(variance + EPSILON)
    groups = [v * inv for v in groups]
    grads = []
    for g in range(4):
        span = slice(features * g, features * (g + 1))
        gain = gain_ref[:, span]
        merged_in_ref[:, span] = (groups[g] * gain).astype(BF)
        grad_in = dot_nt(gm_ref[...], w_merge_ref[span, :]).astype(BF).astype(F32)
        grads.append(grad_in * gain)
    mean_one = sum(jnp.sum(v, axis=-1, keepdims=True) for v in grads) / width
    mean_two = sum(
        jnp.sum(v * h, axis=-1, keepdims=True) for v, h in zip(grads, groups)
    ) / width
    outs = [(v - mean_one - h * mean_two) * inv for v, h in zip(grads, groups)]
    for i in range(pairs):
        piece = jnp.concatenate([v[half * i : half * (i + 1)] for v in outs], axis=0).astype(BF)
        back = dot_nn(from_patch_ref[...], piece).astype(BF)
        grad_mixed_ref[pl.ds(2 * cols * i, 2 * cols), :] = back
    grad_att_ref[...] = dot_nt(grad_mixed_ref[...], w_out_ref[...]).astype(BF)


def merge_grad_kernel(steps, merged_in_ref, gm_ref, att_ref, gmix_ref, out_m_ref, out_o_ref):
    out_m_ref[...] = dot_tn(merged_in_ref[...], gm_ref[...]).astype(BF)
    out_o_ref[...] = dot_tn(att_ref[...], gmix_ref[...]).astype(BF)


def backward_kernel(stride, count_b, steps, ga_ref, allow_ref, qkv_ref, normed_ref, to_win_ref,
                    dwo_ref, gqkv_ref, dw_ref, acc_ref):
    features = ga_ref.shape[1]
    step = pl.program_id(0)
    ga = dot_nn(to_win_ref[...], ga_ref[...]).astype(BF)
    allow = allow_ref[0] > 0.5
    masks = lane_masks()
    for b in range(count_b):
        rows = slice(b * stride, (b + 1) * stride)
        for pair in range(features // 128):
            q2 = qkv_ref[rows, pl.ds(128 * pair, 128)] * jnp.asarray(0.125, BF)
            k2 = qkv_ref[rows, pl.ds(features + 128 * pair, 128)]
            v2 = qkv_ref[rows, pl.ds(2 * features + 128 * pair, 128)]
            do2 = ga[rows, 128 * pair : 128 * pair + 128]
            dq = dk = dv = None
            for m in masks:
                km, dom = k2 * m, do2 * m
                s = jnp.where(allow, dot_nt(km, q2), -1e30)
                s = s - jnp.max(s, axis=0, keepdims=True)
                e = jnp.exp(s)
                p = e / jnp.sum(e, axis=0, keepdims=True)
                dp = dot_nt(v2, dom)
                ds = p * (dp - jnp.sum(dp * p, axis=0, keepdims=True))
                ds = ds.astype(BF)
                dv1 = dot_nn(p.astype(BF), dom)
                dk1 = dot_nn(ds, q2 * m)
                dq1 = dot_tn(ds, km)
                dq, dk, dv = (dq1, dk1, dv1) if dq is None else (dq + dq1, dk + dk1, dv + dv1)
            gqkv_ref[rows, pl.ds(128 * pair, 128)] = (dq * 0.125).astype(BF)
            gqkv_ref[rows, pl.ds(features + 128 * pair, 128)] = dk.astype(BF)
            gqkv_ref[rows, pl.ds(2 * features + 128 * pair, 128)] = dv.astype(BF)
    part = dot_tn(normed_ref[...], gqkv_ref[...])

    @pl.when(step == 0)
    def _():
        acc_ref[...] = part

    @pl.when(step > 0)
    def _():
        acc_ref[...] += part

    @pl.when(step == steps - 1)
    def _():
        dw_ref[:, : 3 * features] = acc_ref[...].astype(BF)
        dw_ref[:, 3 * features :] = dwo_ref[...]


def input_grad_kernel(gqkv_ref, x_ref, gain_ref, w_ref, to_grid_ref, out_ref):
    grad = dot_nt(gqkv_ref[...], w_ref[...]).astype(BF)
    grad = dot_nn(to_grid_ref[...], grad)
    x = x_ref[...].astype(F32)
    centered = x - jnp.mean(x, axis=-1, keepdims=True)
    inv = lax.rsqrt(jnp.mean(centered * centered, axis=-1, keepdims=True) + EPSILON)
    hat = centered * inv
    grad = grad * gain_ref[...]
    one = jnp.mean(grad, axis=-1, keepdims=True)
    two = jnp.mean(grad * hat, axis=-1, keepdims=True)
    out_ref[...] = (grad - one - hat * two) * inv


def merged_kernel(a_ref, w_ref, out_ref):
    out_ref[...] = dot_nn(a_ref[...], w_ref[...]).astype(BF)


def whole(shape):
    return pl.BlockSpec(shape, lambda i: (0,) * len(shape))


def rows_of(height, width):
    return pl.BlockSpec((height, width), lambda i: (i, 0))


def shift_pairs(count_lat, count_lon, dlat, dlon):
    return [
        (a * count_lon + b, ((a + dlat) % count_lat) * count_lon + (b + dlon) % count_lon)
        for a in range(count_lat)
        for b in range(count_lon)
    ]


def send(value, dlat, dlon):
    pairs = shift_pairs(lax.axis_size("lat"), lax.axis_size("lon"), dlat, dlon)
    return lax.ppermute(value, ("lat", "lon"), pairs)


def to_shifted(values):
    rows, cols, _ = values.shape
    hr, hc = WLAT // 2, WLON // 2
    west = send(values[: rows - hr, cols - hc :], 0, 1)
    south = send(values[rows - hr :, : cols - hc], 1, 0)
    corner = send(values[rows - hr :, cols - hc :], 1, 1)
    top = jnp.concatenate([corner, south], axis=1)
    bottom = jnp.concatenate([west, values[: rows - hr, : cols - hc]], axis=1)
    return jnp.concatenate([top, bottom], axis=0)


def from_shifted(values, cast=lambda v: v):
    rows, cols, _ = values.shape
    hr, hc = WLAT // 2, WLON // 2
    east = send(cast(values[hr:, :hc]), 0, -1).astype(values.dtype)
    north = send(cast(values[:hr, hc:]), -1, 0).astype(values.dtype)
    corner = send(cast(values[:hr, :hc]), -1, -1).astype(values.dtype)
    top = jnp.concatenate([values[hr:, hc:], east], axis=1)
    bottom = jnp.concatenate([north, corner], axis=1)
    return jnp.concatenate([top, bottom], axis=0)


def halve(value, keep):
    half = value.shape[0] // 2
    kept = lax.dynamic_slice_in_dim(value, keep * half, half, 0)
    sent = lax.dynamic_slice_in_dim(value, (1 - keep) * half, half, 0)
    return kept, sent


def join(value, received, keep):
    first = jnp.where(keep == 0, value, received)
    second = jnp.where(keep == 0, received, value)
    return jnp.concatenate([first, second], axis=0)


def reduce_all(value):
    count_lat, count_lon = lax.axis_size("lat"), lax.axis_size("lon")
    bits = count_lon.bit_length() - 1
    me, lat = lax.axis_index("lon"), lax.axis_index("lat")
    odd = lax.rem(me, 2)
    plans = [([(i, i ^ 1) for i in range(count_lon)], odd)]
    for k in range(bits - 1):
        low, high = 2 << k, 2 << (bits - 2 - k)
        pairs = [(i, i ^ (low if i % 2 == 0 else high)) for i in range(count_lon)]
        keep = jnp.where(odd == 0, lax.rem(me // low, 2), lax.rem(me // high, 2))
        plans.append((pairs, keep))
    for pairs, keep in plans:
        kept, sent = halve(value, keep)
        received = lax.ppermute(sent, "lon", pairs)
        value = (kept.astype(F32) + received.astype(F32)).astype(BF)
    height = value.shape[0] // count_lat
    total = lax.dynamic_slice_in_dim(value, lat * height, height, 0).astype(F32)
    for d in range(1, count_lat):
        sent = lax.dynamic_slice_in_dim(value, (lat ^ d) * height, height, 0)
        total = total + lax.ppermute(sent, "lat", [(i, i ^ d) for i in range(count_lat)]).astype(F32)
    mine = total.astype(BF)
    value = jnp.zeros((count_lat * height,) + mine.shape[1:], BF)
    value = lax.dynamic_update_slice_in_dim(value, mine, lat * height, 0)
    for d in range(1, count_lat):
        received = lax.ppermute(mine, "lat", [(i, i ^ d) for i in range(count_lat)])
        value = lax.dynamic_update_slice_in_dim(value, received, (lat ^ d) * height, 0)
    for pairs, keep in reversed(plans):
        value = join(value, lax.ppermute(value, "lon", pairs), keep)
    return value


def on_device(tokens, lat_band, gain_attn, w_qkv, w_out, gain_merge, w_merge, grad_merged):
    rows, cols, features = tokens.shape
    width2 = grad_merged.shape[2]
    count_a, count_b = rows // WLAT, cols // WLON
    window = WLAT * WLON
    stride = -(-window // 16) * 16
    half_lat = WLAT // 2
    block = WLAT * cols
    padded = count_b * stride
    total = rows * cols
    to_win_np = window_matrix(cols, stride)
    to_win = jnp.asarray(to_win_np, BF)
    to_grid = jnp.asarray(to_win_np.T, BF)
    patch_np = patch_matrix(cols)
    to_patch = jnp.asarray(patch_np, BF)
    from_patch = jnp.asarray(patch_np.T, BF)

    band_count = lat_band.shape[0]
    extended = jnp.concatenate([lat_band[band_count - half_lat :], lat_band])
    band_rows = lax.dynamic_slice_in_dim(extended, lax.axis_index("lat") * rows, rows)
    labels = jnp.repeat(band_rows.reshape(count_a, WLAT), WLON, axis=1)
    labels = jnp.pad(labels, ((0, 0), (0, stride - window)), constant_values=-1)
    allow = (labels[:, :, None] == labels[:, None, :]).astype(F32)
    gain_a = gain_attn.reshape(1, features)
    gain_m = gain_merge.reshape(1, 4 * features)

    shifted = to_shifted(tokens).reshape(total, features)
    allow_spec = pl.BlockSpec((1, stride, stride), lambda i: (i, 0, 0))
    attended, qkv, normed = pl.pallas_call(
        functools.partial(forward_kernel, stride, count_b),
        grid=(count_a,),
        in_specs=[rows_of(block, features), allow_spec, whole((1, features)),
                  whole((features, 3 * features)), whole((padded, block)), whole((block, padded))],
        out_specs=[rows_of(block, features), rows_of(padded, 3 * features), rows_of(padded, features)],
        out_shape=[jax.ShapeDtypeStruct((total, features), BF),
                   jax.ShapeDtypeStruct((count_a * padded, 3 * features), BF),
                   jax.ShapeDtypeStruct((count_a * padded, features), BF)],
        scratch_shapes=[pltpu.VMEM((padded, features), BF)],
        compiler_params=params(1),
        cost_estimate=cost(4 * total * features * 3 * features, 2 * total * features * 8),
        name="attn_fwd",
    )(shifted, allow, gain_a, w_qkv, to_win, to_grid)

    own_att = from_shifted(attended.reshape(rows, cols, features)).reshape(total, features)
    own_tok = tokens.reshape(total, features)
    gm = grad_merged.reshape(total // 4, width2)

    steps = 2
    tall = total // steps
    short = tall // 4
    merged_in, grad_mixed, grad_att = pl.pallas_call(
        functools.partial(middle_kernel, cols),
        grid=(steps,),
        in_specs=[rows_of(tall, features), rows_of(tall, features), whole((features, features)),
                  whole((1, 4 * features)), whole((4 * features, width2)), rows_of(short, width2),
                  whole((2 * cols, 2 * cols)), whole((2 * cols, 2 * cols))],
        out_specs=[rows_of(short, 4 * features), rows_of(tall, features), rows_of(tall, features)],
        out_shape=[jax.ShapeDtypeStruct((total // 4, 4 * features), BF),
                   jax.ShapeDtypeStruct((total, features), BF),
                   jax.ShapeDtypeStruct((total, features), BF)],
        compiler_params=params(1),
        cost_estimate=cost(8 * total * features * features, 2 * total * features * 6),
        name="merge_mid",
    )(own_tok, own_att, w_out, gain_m, w_merge, gm, to_patch, from_patch)

    pieces = 4
    dw_merge, dw_out = pl.pallas_call(
        functools.partial(merge_grad_kernel, pieces),
        grid=(pieces,),
        in_specs=[pl.BlockSpec((total // 4, 4 * features // pieces), lambda i: (0, i)),
                  whole((total // 4, width2)),
                  pl.BlockSpec((total, features // pieces), lambda i: (0, i)),
                  whole((total, features))],
        out_specs=[rows_of(4 * features // pieces, width2), rows_of(features // pieces, features)],
        out_shape=[jax.ShapeDtypeStruct((4 * features, width2), BF),
                   jax.ShapeDtypeStruct((features, features), BF)],
        compiler_params=params(1),
        cost_estimate=cost(4 * total * features * features * 2, 2 * total * features * 6),
        name="merge_dw",
    )(merged_in, gm, own_att, grad_mixed)
    sum_merge = reduce_all(dw_merge)

    grad_shifted = to_shifted(grad_att.reshape(rows, cols, features)).reshape(total, features)
    grad_qkv, dw_q = pl.pallas_call(
        functools.partial(backward_kernel, stride, count_b, count_a),
        grid=(count_a,),
        in_specs=[rows_of(block, features), allow_spec, rows_of(padded, 3 * features),
                  rows_of(padded, features), whole((padded, block)), whole((features, features))],
        out_specs=[rows_of(padded, 3 * features), whole((features, 4 * features))],
        out_shape=[jax.ShapeDtypeStruct((count_a * padded, 3 * features), BF),
                   jax.ShapeDtypeStruct((features, 4 * features), BF)],
        scratch_shapes=[pltpu.VMEM((features, 3 * features), F32)],
        compiler_params=params(1),
        cost_estimate=cost(4 * total * features * 3 * features, 2 * total * features * 8),
        name="attn_bwd",
    )(grad_shifted, allow, qkv, normed, to_win, dw_out)
    sum_q = reduce_all(dw_q)

    grad_inputs = pl.pallas_call(
        input_grad_kernel,
        grid=(count_a,),
        in_specs=[rows_of(padded, 3 * features), rows_of(block, features), whole((1, features)),
                  whole((features, 3 * features)), whole((block, padded))],
        out_specs=rows_of(block, features),
        out_shape=jax.ShapeDtypeStruct((total, features), F32),
        compiler_params=params(1),
        cost_estimate=cost(2 * total * features * 3 * features, 2 * total * features * 6),
        name="input_grad",
    )(grad_qkv, shifted, gain_a, w_qkv, to_grid)
    grad_own = from_shifted(grad_inputs.reshape(rows, cols, features), lambda v: v.astype(BF))
    grad_tokens = grad_own + grad_mixed.reshape(rows, cols, features).astype(F32)

    merged = pl.pallas_call(
        merged_kernel,
        grid=(2,),
        in_specs=[rows_of(total // 8, 4 * features), whole((4 * features, width2))],
        out_specs=rows_of(total // 8, width2),
        out_shape=jax.ShapeDtypeStruct((total // 4, width2), BF),
        compiler_params=params(1),
        cost_estimate=cost(2 * total * features * width2, 2 * total * features * 4),
        name="merged",
    )(merged_in, w_merge).reshape(grad_merged.shape)

    grad_w_merge = sum_merge.astype(F32)
    grad_w_qkv = sum_q[:, : 3 * features].astype(F32)
    grad_w_out = sum_q[:, 3 * features :].astype(F32)
    grad_gain_merge = jnp.sum(grad_w_merge * w_merge.astype(F32), axis=1) / gain_merge
    grad_gain_attn = jnp.sum(grad_w_qkv * w_qkv.astype(F32), axis=1) / gain_attn
    return (merged, grad_tokens, grad_gain_attn, grad_w_qkv, grad_w_out, grad_gain_merge,
            grad_w_merge)


def solution(mesh):
    return jax.shard_map(
        on_device,
        mesh=mesh,
        in_specs=(P("lat", "lon", None), P(), P(), P(), P(), P(), P(), P("lat", "lon", None)),
        out_specs=(P("lat", "lon", None), P("lat", "lon", None), P(), P(), P(), P(), P()),
        check_vma=False,
    )
```

```python
import functools

import jax
import jax.numpy as jnp
import numpy as np
from jax import lax
from jax.experimental import pallas as pl
from jax.experimental.pallas import tpu as pltpu
from jax.sharding import PartitionSpec as P


WLAT = 6
WLON = 12
EPSILON = 1e-05
EDGE = 8
BF = jnp.bfloat16
F32 = jnp.float32

CALLS = 4


def dot_nn(a, b):
    return lax.dot_general(a, b, (((1,), (0,)), ((), ())), preferred_element_type=F32)


def dot_nt(a, b):
    return lax.dot_general(a, b, (((1,), (1,)), ((), ())), preferred_element_type=F32)


def dot_tn(a, b):
    return lax.dot_general(a, b, (((0,), (0,)), ((), ())), preferred_element_type=F32)


def params(steps):
    return pltpu.CompilerParams(
        dimension_semantics=("arbitrary",) * steps, vmem_limit_bytes=60 * 1024 * 1024
    )


def cost(flops, nbytes):
    return pl.CostEstimate(flops=int(flops), transcendentals=0, bytes_accessed=int(nbytes))


def window_matrix(cols, stride):
    count_b = cols // WLON
    mat = np.zeros((count_b * stride, WLAT * cols), np.float32)
    for b in range(count_b):
        for r in range(WLAT):
            for c in range(WLON):
                mat[b * stride + r * WLON + c, r * cols + b * WLON + c] = 1.0
    return mat


def halo_matrices(rows, cols, stride):
    hr, hc = WLAT // 2, WLON // 2
    count_a, count_b = rows // WLAT, cols // WLON
    padded = count_b * stride
    own = np.zeros((2, padded, WLAT * cols), np.float32)
    west = np.zeros((count_a, padded, rows * EDGE), np.float32)
    south = np.zeros((padded, hr * cols), np.float32)
    corner = np.zeros((padded, hr * EDGE), np.float32)
    for a in range(count_a):
        for b in range(count_b):
            for r in range(WLAT):
                for c in range(WLON):
                    place = b * stride + r * WLON + c
                    row, col = a * WLAT + r - hr, b * WLON + c - hc
                    if row >= 0 and col >= 0:
                        base = row if a == 0 else r
                        own[min(a, 1), place, base * cols + col] = 1.0
                    elif row >= 0:
                        west[a, place, row * EDGE + col + EDGE] = 1.0
                    elif col >= 0:
                        south[place, (row + hr) * cols + col] = 1.0
                    else:
                        corner[place, (row + hr) * EDGE + col + EDGE] = 1.0
    return [jnp.asarray(m, BF) for m in (own, west, south, corner)]


def patch_matrix(cols):
    half = cols // 2
    mat = np.zeros((4 * half, 2 * cols), np.float32)
    for j in range(half):
        for g, (dr, dc) in enumerate(((0, 0), (1, 0), (0, 1), (1, 1))):
            mat[g * half + j, dr * cols + 2 * j + dc] = 1.0
    return mat


def lane_masks():
    lane = lax.broadcasted_iota(jnp.int32, (1, 128), 1)
    even = (lane < 64).astype(F32)
    return even.astype(BF), (1.0 - even).astype(BF)


def halo_rows(own_ref, west_ref, south_ref, corner_ref, po_ref, pw_ref, ps_ref, pc_ref, first):
    step = pl.program_id(0)
    block = po_ref.shape[2]
    half = block // 2
    start = pl.multiple_of(jnp.maximum(step * block - half, 0), 16)
    take = jnp.where(step == 0, 0, 1)
    value = dot_nn(po_ref[take], own_ref[pl.ds(start, block), :])
    value = value + dot_nn(pw_ref[0], west_ref[...])
    first[...] = value

    @pl.when(step == 0)
    def _():
        first[...] += dot_nn(ps_ref[...], south_ref[...]) + dot_nn(pc_ref[...], corner_ref[...])

    return first[...]


def stack_heads(value, masks):
    return jnp.concatenate([value * masks[0], value * masks[1]], axis=0)


def forward_kernel(stride, count_b, own_ref, west_ref, south_ref, corner_ref, po_ref, pw_ref, ps_ref,
                   pc_ref, allow_ref, gain_ref, w_ref, to_grid_ref,
                   att_ref, qkv_ref, normed_ref, prob_ref, lon_ref, lat_ref, corner_out_ref, first,
                   att_win_ref):
    features = own_ref.shape[1]
    x = halo_rows(own_ref, west_ref, south_ref, corner_ref, po_ref, pw_ref, ps_ref, pc_ref, first)
    average = jnp.mean(x, axis=-1, keepdims=True)
    centered = x - average
    variance = jnp.mean(centered * centered, axis=-1, keepdims=True)
    normed = (centered * lax.rsqrt(variance + EPSILON) * gain_ref[...]).astype(BF)
    normed_ref[...] = normed
    for t in range(3):
        qkv_ref[t] = dot_nn(normed, w_ref[:, features * t : features * (t + 1)]).astype(BF)
    allow = allow_ref[0] > 0.5
    masks = lane_masks()
    spans = [slice(b * stride, (b + 1) * stride) for b in range(count_b)]
    for pair in range(features // 128):
        lanes = pl.ds(128 * pair, 128)
        scores = []
        for rows in spans:
            q2 = qkv_ref[0, rows, lanes] * jnp.asarray(0.125, BF)
            scores.append(dot_nt(stack_heads(qkv_ref[1, rows, lanes], masks), q2))
        stacked = []
        for b, s2 in enumerate(scores):
            probs = []
            for h in range(2):
                s = jnp.where(allow, s2[h * stride : (h + 1) * stride], -1e30)
                e = jnp.exp(s - jnp.max(s, axis=0, keepdims=True))
                probs.append((e * (1.0 / jnp.sum(e, axis=0, keepdims=True))).astype(BF))
            p2 = jnp.concatenate(probs, axis=0)
            prob_ref[pair, pl.ds(2 * stride * b, 2 * stride), :] = p2
            stacked.append(p2)
        for rows, p2 in zip(spans, stacked):
            o2 = dot_tn(p2, stack_heads(qkv_ref[2, rows, lanes], masks))
            att_win_ref[rows, lanes] = o2.astype(BF)
    write_edges(dot_nn(to_grid_ref[...], att_win_ref[...]), att_ref, lon_ref, lat_ref, corner_out_ref)


def write_edges(values, out_ref, lon_ref, lat_ref, corner_ref):
    cols = values.shape[0] // WLAT
    out_ref[...] = values.astype(out_ref.dtype)
    edge = jnp.concatenate([values[r * cols : r * cols + EDGE] for r in range(WLAT)], axis=0).astype(BF)
    lon_ref[...] = edge

    @pl.when(pl.program_id(0) == 0)
    def _():
        lat_ref[...] = values[: lat_ref.shape[0]].astype(BF)
        corner_ref[...] = edge[: corner_ref.shape[0]]


def assemble_kernel(own_ref, west_ref, south_ref, corner_ref, po_ref, pw_ref, ps_ref, pc_ref, out_ref,
                    first):
    out_ref[...] = halo_rows(own_ref, west_ref, south_ref, corner_ref, po_ref, pw_ref, ps_ref, pc_ref,
                             first).astype(BF)


def middle_kernel(cols, tok_ref, att_ref, w_out_ref, gain_ref, grad_in_ref, to_patch_ref,
                  from_patch_ref, merged_in_ref, grad_mixed_ref, grad_att_ref, lon_ref, lat_ref,
                  corner_ref):
    tokens, features = tok_ref.shape
    pairs = tokens // (2 * cols)
    half = cols // 2
    mixed = (tok_ref[...].astype(F32) + dot_nn(att_ref[...], w_out_ref[...])).astype(BF)
    parts = [dot_nn(to_patch_ref[...], mixed[2 * cols * i : 2 * cols * (i + 1)]) for i in range(pairs)]
    groups = [
        jnp.concatenate([part[half * g : half * (g + 1)] for part in parts], axis=0) for g in range(4)
    ]
    width = 4 * features
    average = sum(jnp.sum(v, axis=-1, keepdims=True) for v in groups) / width
    groups = [v - average for v in groups]
    variance = sum(jnp.sum(v * v, axis=-1, keepdims=True) for v in groups) / width
    inv = lax.rsqrt(variance + EPSILON)
    groups = [v * inv for v in groups]
    grads = []
    for g in range(4):
        span = slice(features * g, features * (g + 1))
        gain = gain_ref[:, span]
        merged_in_ref[:, span] = (groups[g] * gain).astype(BF)
        grads.append(grad_in_ref[:, span].astype(F32) * gain)
    mean_one = sum(jnp.sum(v, axis=-1, keepdims=True) for v in grads) / width
    mean_two = sum(
        jnp.sum(v * h, axis=-1, keepdims=True) for v, h in zip(grads, groups)
    ) / width
    outs = [(v - mean_one - h * mean_two) * inv for v, h in zip(grads, groups)]
    for i in range(pairs):
        piece = jnp.concatenate([v[half * i : half * (i + 1)] for v in outs], axis=0).astype(BF)
        back = dot_nn(from_patch_ref[...], piece).astype(BF)
        grad_mixed_ref[pl.ds(2 * cols * i, 2 * cols), :] = back
    grad_att = dot_nt(grad_mixed_ref[...], w_out_ref[...])
    grad_att_ref[...] = grad_att.astype(BF)
    edge = [grad_att[r * cols - EDGE : r * cols] for r in range(1, tokens // cols + 1)]
    lon_ref[...] = jnp.concatenate(edge, axis=0).astype(BF)

    @pl.when(pl.program_id(0) == pl.num_programs(0) - 1)
    def _():
        lat_ref[...] = grad_att[tokens - lat_ref.shape[0] :].astype(BF)
        corner_ref[...] = jnp.concatenate(edge[-(WLAT // 2) :], axis=0).astype(BF)


def grad_in_kernel(gm_ref, w_merge_ref, out_ref):
    out_ref[...] = dot_nt(gm_ref[...], w_merge_ref[...]).astype(BF)


def merge_grad_kernel(merged_in_ref, gm_ref, att_ref, gmix_ref, out_ref):
    step = pl.program_id(0)
    last = pl.num_programs(0) - 1
    height = out_ref.shape[0]
    narrow = gmix_ref.shape[1]

    @pl.when(step < last)
    def _():
        out_ref[...] = dot_tn(merged_in_ref[...], gm_ref[...]).astype(BF)

    @pl.when(step == last)
    def _():
        for k in range(att_ref.shape[1] // height):
            part = dot_tn(att_ref[:, height * k : height * (k + 1)], gmix_ref[...])
            out_ref[:, narrow * k : narrow * (k + 1)] = part.astype(BF)


def backward_kernel(stride, count_b, ga_ref, qkv_ref, prob_ref, prev_ref, gqkv_ref):
    del prev_ref
    masks = lane_masks()
    low = lax.broadcasted_iota(jnp.int32, (1, 128), 1) < 64
    spans = [slice(b * stride, (b + 1) * stride) for b in range(count_b)]
    for pair in range(ga_ref.shape[1] // 128):
        lanes = pl.ds(128 * pair, 128)
        work = []
        for b, rows in enumerate(spans):
            do2 = ga_ref[rows, lanes]
            p2 = prob_ref[pair, pl.ds(2 * stride * b, 2 * stride), :]
            dp2 = dot_nt(stack_heads(qkv_ref[2, rows, lanes], masks), do2)
            dv = dot_nn(p2, do2)
            gqkv_ref[2, rows, lanes] = jnp.where(low, dv[:stride], dv[stride:]).astype(BF)
            work.append((p2, dp2))
        scores = []
        for p2, dp2 in work:
            grads = []
            for h in range(2):
                p = p2[h * stride : (h + 1) * stride].astype(F32)
                dp = dp2[h * stride : (h + 1) * stride]
                grads.append((p * (dp - jnp.sum(dp * p, axis=0, keepdims=True))).astype(BF))
            scores.append(jnp.concatenate(grads, axis=0))
        for rows, ds2 in zip(spans, scores):
            q2 = qkv_ref[0, rows, lanes] * jnp.asarray(0.125, BF)
            dk = dot_nn(ds2, q2)
            dq = dot_tn(ds2, stack_heads(qkv_ref[1, rows, lanes], masks))
            gqkv_ref[0, rows, lanes] = (dq * 0.125).astype(BF)
            gqkv_ref[1, rows, lanes] = jnp.where(low, dk[:stride], dk[stride:]).astype(BF)


def qkv_grad_kernel(normed_ref, gqkv_ref, out_ref):
    for t in range(3):
        out_ref[t] = dot_tn(normed_ref[...], gqkv_ref[t]).astype(BF)


def input_grad_kernel(gqkv_ref, x_ref, gain_ref, w_ref, to_grid_ref, out_ref, lon_ref, lat_ref,
                      corner_ref):
    features = x_ref.shape[1]
    grad = sum(dot_nt(gqkv_ref[t], w_ref[:, features * t : features * (t + 1)]) for t in range(3))
    grad = dot_nn(to_grid_ref[...], grad.astype(BF))
    x = x_ref[...].astype(F32)
    centered = x - jnp.mean(x, axis=-1, keepdims=True)
    inv = lax.rsqrt(jnp.mean(centered * centered, axis=-1, keepdims=True) + EPSILON)
    hat = centered * inv
    grad = grad * gain_ref[...]
    one = jnp.mean(grad, axis=-1, keepdims=True)
    two = jnp.mean(grad * hat, axis=-1, keepdims=True)
    write_edges((grad - one - hat * two) * inv, out_ref, lon_ref, lat_ref, corner_ref)


def merged_kernel(a_ref, w_ref, out_ref):
    out_ref[...] = dot_nn(a_ref[...], w_ref[...]).astype(BF)


def whole(shape):
    return pl.BlockSpec(shape, lambda i: (0,) * len(shape))


def rows_of(height, width):
    return pl.BlockSpec((height, width), lambda i: (i, 0))


def shift_pairs(count_lat, count_lon, dlat, dlon):
    return [
        (a * count_lon + b, ((a + dlat) % count_lat) * count_lon + (b + dlon) % count_lon)
        for a in range(count_lat)
        for b in range(count_lon)
    ]


def send(value, dlat, dlon):
    pairs = shift_pairs(lax.axis_size("lat"), lax.axis_size("lon"), dlat, dlon)
    return lax.ppermute(value, ("lat", "lon"), pairs)


def exchange(parts, sign):
    lon_edge, lat_edge, corner = parts
    lon_edge = send(lon_edge, 0, sign)
    lat_edge = send(lat_edge, sign, 0)
    corner = send(corner, sign, sign)
    return lon_edge, lat_edge, corner


def edges(values):
    rows, cols, features = values.shape
    hr = WLAT // 2
    parts = (values[:, cols - EDGE :], values[rows - hr :], values[rows - hr :, cols - EDGE :])
    return [v.reshape(-1, features) for v in parts]


def to_shifted(values, parts):
    rows, cols, features = values.shape
    hr, hc = WLAT // 2, WLON // 2
    west, south, corner = parts
    corner = corner.reshape(hr, EDGE, features)[:, EDGE - hc :]
    top = jnp.concatenate([corner, south.reshape(hr, cols, features)[:, : cols - hc]], 1)
    west = west.reshape(rows, EDGE, features)[: rows - hr, EDGE - hc :]
    bottom = jnp.concatenate([west, values[: rows - hr, : cols - hc]], 1)
    return jnp.concatenate([top, bottom], axis=0)


def to_own(values, parts):
    rows, cols, features = values.shape
    hr, hc = WLAT // 2, WLON // 2
    east, north, corner = (v.astype(values.dtype) for v in parts)
    top = jnp.concatenate([values[hr:, hc:], east.reshape(rows, EDGE, features)[hr:, :hc]], axis=1)
    north = north.reshape(hr, cols, features)[:, hc:]
    bottom = jnp.concatenate([north, corner.reshape(hr, EDGE, features)[:, :hc]], axis=1)
    return jnp.concatenate([top, bottom], axis=0)


def part_sum(terms, index, height):
    parts = [lax.dynamic_slice_in_dim(t, index * height, height, 0).astype(F32) for t in terms]
    return sum(parts[1:], parts[0]).astype(BF)


def join(value, received, keep):
    first = jnp.where(keep == 0, value, received)
    second = jnp.where(keep == 0, received, value)
    return jnp.concatenate([first, second], axis=0)


def reduce_all(value):
    count_lat, count_lon = lax.axis_size("lat"), lax.axis_size("lon")
    bits = count_lon.bit_length() - 1
    me, lat = lax.axis_index("lon"), lax.axis_index("lat")
    odd = lax.rem(me, 2)
    plans = [([(i, i ^ 1) for i in range(count_lon)], odd)]
    for k in range(bits - 1):
        low, high = 2 << k, 2 << (bits - 2 - k)
        pairs = [(i, i ^ (low if i % 2 == 0 else high)) for i in range(count_lon)]
        keep = jnp.where(odd == 0, lax.rem(me // low, 2), lax.rem(me // high, 2))
        plans.append((pairs, keep))
    terms, height = [value], value.shape[0]
    for pairs, keep in plans:
        height = height // 2
        sent = part_sum(terms, 1 - keep, height)
        received = lax.ppermute(sent, "lon", pairs)
        terms = [lax.dynamic_slice_in_dim(t, keep * height, height, 0) for t in terms] + [received]
    height = height // count_lat
    total = [lax.dynamic_slice_in_dim(t, lat * height, height, 0).astype(F32) for t in terms]
    for d in range(1, count_lat):
        sent = part_sum(terms, lat ^ d, height)
        received = lax.ppermute(sent, "lat", [(i, i ^ d) for i in range(count_lat)])
        total.append(received.astype(F32))
    mine = sum(total[1:], total[0]).astype(BF)
    value = jnp.zeros((count_lat * height,) + mine.shape[1:], BF)
    value = lax.dynamic_update_slice_in_dim(value, mine, lat * height, 0)
    for d in range(1, count_lat):
        received = lax.ppermute(mine, "lat", [(i, i ^ d) for i in range(count_lat)])
        value = lax.dynamic_update_slice_in_dim(value, received, (lat ^ d) * height, 0)
    for k, (pairs, keep) in reversed(list(enumerate(plans))):
        received = lax.ppermute(value, "lon", pairs)
        value = join(value, received, keep)
    return value


def on_device_body(tokens, lat_band, gain_attn, w_qkv, w_out, gain_merge, w_merge, grad_merged):
    rows, cols, features = tokens.shape
    width2 = grad_merged.shape[2]
    count_a, count_b = rows // WLAT, cols // WLON
    window = WLAT * WLON
    stride = -(-window // 16) * 16
    half_lat = WLAT // 2
    block = WLAT * cols
    padded = count_b * stride
    total = rows * cols
    to_grid = jnp.asarray(window_matrix(cols, stride).T, BF)
    patch_np = patch_matrix(cols)
    to_patch = jnp.asarray(patch_np, BF)
    from_patch = jnp.asarray(patch_np.T, BF)

    band_count = lat_band.shape[0]
    extended = jnp.concatenate([lat_band[band_count - half_lat :], lat_band])
    band_rows = lax.dynamic_slice_in_dim(extended, lax.axis_index("lat") * rows, rows)
    labels = jnp.repeat(band_rows.reshape(count_a, WLAT), WLON, axis=1)
    labels = jnp.pad(labels, ((0, 0), (0, stride - window)), constant_values=-1)
    allow = (labels[:, :, None] == labels[:, None, :]).astype(F32)
    gain_a = gain_attn.reshape(1, features)
    gain_m = gain_merge.reshape(1, 4 * features)

    own_tok = tokens.reshape(total, features)
    mats = halo_matrices(rows, cols, stride)
    edge_shapes = [(rows * EDGE, features), (half_lat * cols, features), (half_lat * EDGE, features)]
    edge_types = [jax.ShapeDtypeStruct(shape, BF) for shape in edge_shapes]
    edge_specs = [rows_of(WLAT * EDGE, features), whole(edge_shapes[1]), whole(edge_shapes[2])]
    halo_specs = [whole((total, features))] + [whole(shape) for shape in edge_shapes] + [
        whole(mats[0].shape), pl.BlockSpec((1,) + mats[1].shape[1:], lambda i: (i, 0, 0)),
        whole(mats[2].shape), whole(mats[3].shape)]
    tok_halos = exchange(edges(tokens), 1)
    allow_spec = pl.BlockSpec((1, stride, stride), lambda i: (i, 0, 0))
    pairs = features // 128
    tall3 = count_a * padded
    qkv_spec = pl.BlockSpec((3, padded, features), lambda i: (0, i, 0))
    prob_rows = 2 * stride * count_b
    attended, qkv, normed, probs, *att_edges = pl.pallas_call(
        functools.partial(forward_kernel, stride, count_b),
        grid=(count_a,),
        in_specs=halo_specs + [allow_spec, whole((1, features)), whole((features, 3 * features)),
                               whole((block, padded))],
        out_specs=[rows_of(block, features), qkv_spec, rows_of(padded, features),
                   pl.BlockSpec((pairs, prob_rows, stride), lambda i: (0, i, 0))] + edge_specs,
        out_shape=[jax.ShapeDtypeStruct((total, features), BF),
                   jax.ShapeDtypeStruct((3, tall3, features), BF),
                   jax.ShapeDtypeStruct((tall3, features), BF),
                   jax.ShapeDtypeStruct((pairs, count_a * prob_rows, stride), BF)] + edge_types,
        scratch_shapes=[pltpu.VMEM((padded, features), F32), pltpu.VMEM((padded, features), BF)],
        compiler_params=params(1),
        cost_estimate=cost(4 * total * features * 3 * features, 2 * total * features * 8),
        name="attn_fwd",
    )(own_tok, *tok_halos, *mats, allow, gain_a, w_qkv, to_grid)

    att_parts = exchange(att_edges, -1)
    own_att = to_own(attended.reshape(rows, cols, features), att_parts).reshape(total, features)
    gm = grad_merged.reshape(total // 4, width2)
    grad_in = pl.pallas_call(
        grad_in_kernel,
        grid=(4,),
        in_specs=[whole((total // 4, width2)), rows_of(features, width2)],
        out_specs=pl.BlockSpec((total // 4, features), lambda i: (0, i)),
        out_shape=jax.ShapeDtypeStruct((total // 4, 4 * features), BF),
        compiler_params=params(1),
        cost_estimate=cost(2 * total * features * width2, 2 * total * features * 4),
        name="grad_in",
    )(gm, w_merge)

    steps = 2
    tall = total // steps
    short = tall // 4
    merged_in, grad_mixed, grad_att, *grad_edges = pl.pallas_call(
        functools.partial(middle_kernel, cols),
        grid=(steps,),
        in_specs=[rows_of(tall, features), rows_of(tall, features), whole((features, features)),
                  whole((1, 4 * features)), rows_of(short, 4 * features),
                  whole((2 * cols, 2 * cols)), whole((2 * cols, 2 * cols))],
        out_specs=[rows_of(short, 4 * features), rows_of(tall, features), rows_of(tall, features),
                   rows_of(edge_shapes[0][0] // steps, features)] + edge_specs[1:],
        out_shape=[jax.ShapeDtypeStruct((total // 4, 4 * features), BF),
                   jax.ShapeDtypeStruct((total, features), BF),
                   jax.ShapeDtypeStruct((total, features), BF)] + edge_types,
        compiler_params=params(1),
        cost_estimate=cost(8 * total * features * features, 2 * total * features * 6),
        name="merge_mid",
    )(own_tok, own_att, w_out, gain_m, grad_in, to_patch, from_patch)

    att_halos = exchange(grad_edges, 1)
    rest = features * features // width2
    pieces = 4 * features // rest
    dw_merge = pl.pallas_call(
        merge_grad_kernel,
        grid=(pieces + 1,),
        in_specs=[pl.BlockSpec((total // 4, rest), lambda i: (0, jnp.minimum(i, pieces - 1))),
                  whole((total // 4, width2)), whole((total, features)), whole((total, features))],
        out_specs=rows_of(rest, width2),
        out_shape=jax.ShapeDtypeStruct((4 * features + rest, width2), BF),
        compiler_params=params(1),
        cost_estimate=cost(4 * total * features * features * 2, 2 * total * features * 6),
        name="merge_dw",
    )(merged_in, gm, own_att, grad_mixed)
    sum_merge = reduce_all(dw_merge)

    grad_win = pl.pallas_call(
        assemble_kernel,
        grid=(count_a,),
        in_specs=halo_specs,
        out_specs=rows_of(padded, features),
        out_shape=jax.ShapeDtypeStruct((tall3, features), BF),
        scratch_shapes=[pltpu.VMEM((padded, features), F32)],
        compiler_params=params(1),
        cost_estimate=cost(total * features * 1200, 2 * total * features * 3),
        name="assemble",
    )(grad_att, *att_halos, *mats)
    calls = CALLS
    wide = features // calls
    grad_qkv = None
    for j in range(calls):
        spec = pl.BlockSpec((3, padded, wide), lambda i, j=j: (0, i, j))
        operands = [grad_win, qkv, probs]
        specs = [pl.BlockSpec((padded, wide), lambda i, j=j: (i, j)), spec,
                 pl.BlockSpec((pairs // calls, prob_rows, stride), lambda i, j=j: (j, i, 0))]
        if grad_qkv is not None:
            operands.append(grad_qkv)
            specs.append(pl.BlockSpec(memory_space=pl.ANY))
            body = functools.partial(backward_kernel, stride, count_b)
        else:
            def body(ga_ref, qkv_ref, prob_ref, gqkv_ref):
                backward_kernel(stride, count_b, ga_ref, qkv_ref, prob_ref, None, gqkv_ref)
        grad_qkv = pl.pallas_call(
            body,
            grid=(count_a,),
            in_specs=specs,
            out_specs=spec,
            out_shape=jax.ShapeDtypeStruct((3, tall3, features), BF),
            input_output_aliases={3: 0} if j else {},
            compiler_params=params(1),
            cost_estimate=cost(4 * total * features * 3 * features // calls,
                               2 * total * features * 8 // calls),
        )(*operands)
    dw_q = pl.pallas_call(
        qkv_grad_kernel,
        grid=(2,),
        in_specs=[pl.BlockSpec((tall3, features // 2), lambda i: (0, i)),
                  whole((3, tall3, features))],
        out_specs=pl.BlockSpec((3, features // 2, features), lambda i: (0, i, 0)),
        out_shape=jax.ShapeDtypeStruct((3, features, features), BF),
        compiler_params=params(1),
        cost_estimate=cost(2 * total * features * 3 * features, 2 * total * features * 5),
        name="qkv_dw",
    )(normed, grad_qkv)
    sum_q = reduce_all(dw_q.reshape(3 * features, features)).reshape(3, features, features)

    shifted = to_shifted(tokens, tok_halos).reshape(total, features)
    grad_inputs, *in_edges = pl.pallas_call(
        input_grad_kernel,
        grid=(count_a,),
        in_specs=[qkv_spec, rows_of(block, features), whole((1, features)),
                  whole((features, 3 * features)), whole((block, padded))],
        out_specs=[rows_of(block, features)] + edge_specs,
        out_shape=[jax.ShapeDtypeStruct((total, features), F32)] + edge_types,
        compiler_params=params(1),
        cost_estimate=cost(2 * total * features * 3 * features, 2 * total * features * 6),
        name="input_grad",
    )(grad_qkv, shifted, gain_a, w_qkv, to_grid)
    in_parts = exchange(in_edges, -1)
    grad_own = to_own(grad_inputs.reshape(rows, cols, features), in_parts)
    grad_tokens = grad_own + grad_mixed.reshape(rows, cols, features).astype(F32)

    merged = pl.pallas_call(
        merged_kernel,
        grid=(2,),
        in_specs=[rows_of(total // 8, 4 * features), whole((4 * features, width2))],
        out_specs=rows_of(total // 8, width2),
        out_shape=jax.ShapeDtypeStruct((total // 4, width2), BF),
        compiler_params=params(1),
        cost_estimate=cost(2 * total * features * width2, 2 * total * features * 4),
        name="merged",
    )(merged_in, w_merge).reshape(grad_merged.shape)

    grad_w_merge = sum_merge[: 4 * features].astype(F32)
    grad_w_out = jnp.concatenate(
        [sum_merge[4 * features :, k * features : (k + 1) * features] for k in range(features // rest)], 0
    ).astype(F32)
    grad_w_qkv = jnp.concatenate([sum_q[t] for t in range(3)], axis=1).astype(F32)
    grad_gain_merge = jnp.sum(grad_w_merge * w_merge.astype(F32), axis=1) / gain_merge
    grad_gain_attn = jnp.sum(grad_w_qkv * w_qkv.astype(F32), axis=1) / gain_attn
    return (merged, grad_tokens, grad_gain_attn, grad_w_qkv, grad_w_out, grad_gain_merge,
            grad_w_merge)


def solution(mesh):
    return jax.shard_map(
        on_device_body,
        mesh=mesh,
        in_specs=(P("lat", "lon", None), P(), P(), P(), P(), P(), P(), P("lat", "lon", None)),
        out_specs=(P("lat", "lon", None), P("lat", "lon", None), P(), P(), P(), P(), P()),
        check_vma=False,
    )
```

```python
import functools

import jax
import jax.numpy as jnp
import numpy as np
from jax import lax
from jax.experimental import pallas as pl
from jax.experimental.pallas import tpu as pltpu
from jax.sharding import PartitionSpec as P


WLAT = 6
WLON = 12
EPSILON = 1e-05
EDGE = 8
BF = jnp.bfloat16
F32 = jnp.float32

CALLS = 4


def dot_nn(a, b):
    return lax.dot_general(a, b, (((1,), (0,)), ((), ())), preferred_element_type=F32)


def dot_nt(a, b):
    return lax.dot_general(a, b, (((1,), (1,)), ((), ())), preferred_element_type=F32)


def dot_tn(a, b):
    return lax.dot_general(a, b, (((0,), (0,)), ((), ())), preferred_element_type=F32)


def params(steps):
    return pltpu.CompilerParams(
        dimension_semantics=("arbitrary",) * steps, vmem_limit_bytes=60 * 1024 * 1024
    )


def cost(flops, nbytes):
    return pl.CostEstimate(flops=int(flops), transcendentals=0, bytes_accessed=int(nbytes))


def patch_matrix(cols):
    half = cols // 2
    mat = np.zeros((4 * half, 2 * cols), np.float32)
    for j in range(half):
        for g, (dr, dc) in enumerate(((0, 0), (1, 0), (0, 1), (1, 1))):
            mat[g * half + j, dr * cols + 2 * j + dc] = 1.0
    return mat


def lane_masks():
    lane = lax.broadcasted_iota(jnp.int32, (1, 128), 1)
    even = (lane < 64).astype(F32)
    return even.astype(BF), (1.0 - even).astype(BF)


def load_windows(own_ref, west_ref, south_ref, corner_ref, buf_ref, win_ref, stride):
    step = pl.program_id(0)
    cols = south_ref.shape[0] // (WLAT // 2)
    wide = EDGE + cols
    half = WLAT // 2

    def put(r, edge, line):
        buf_ref[pl.ds(wide * r, EDGE), :] = edge.astype(F32)
        buf_ref[pl.ds(wide * r + EDGE, cols), :] = line.astype(F32)

    @pl.when(step == 0)
    def _():
        for r in range(half):
            put(r, corner_ref[r], south_ref[pl.ds(cols * r, cols), :])

    @pl.when(step > 0)
    def _():
        for r in range(half):
            row = WLAT * step - half + r
            put(r, west_ref[row], own_ref[pl.ds(pl.multiple_of(cols * row, 16), cols), :])

    for r in range(half, WLAT):
        row = WLAT * step - half + r
        put(r, west_ref[row], own_ref[pl.ds(pl.multiple_of(cols * row, 16), cols), :])
    for b in range(cols // WLON):
        for r in range(WLAT):
            piece = buf_ref[pl.ds(wide * r + EDGE - WLON // 2 + WLON * b, WLON), :]
            win_ref[pl.ds(stride * b + WLON * r, WLON), :] = piece
        pad = stride - WLAT * WLON
        win_ref[pl.ds(stride * (b + 1) - pad, pad), :] = jnp.zeros((pad, win_ref.shape[1]), F32)


def unload_windows(win_ref, grid_ref, stride):
    cols = grid_ref.shape[0] // WLAT
    for b in range(cols // WLON):
        for r in range(WLAT):
            piece = win_ref[pl.ds(stride * b + WLON * r, WLON), :]
            grid_ref[pl.ds(cols * r + WLON * b, WLON), :] = piece
    return grid_ref[...]


def stack_heads(value, masks):
    return jnp.concatenate([value * masks[0], value * masks[1]], axis=0)


def forward_kernel(stride, count_b, own_ref, west_ref, south_ref, corner_ref, allow_ref, gain_ref,
                   w_ref, att_ref, qkv_ref, normed_ref, tok_ref, prob_ref, lon_ref, lat_ref,
                   corner_out_ref, buf_ref, win_ref, grid_ref):
    features = own_ref.shape[1]
    load_windows(own_ref, west_ref, south_ref, corner_ref, buf_ref, win_ref, stride)
    x = win_ref[...]
    tok_ref[...] = x.astype(BF)
    average = jnp.mean(x, axis=-1, keepdims=True)
    centered = x - average
    variance = jnp.mean(centered * centered, axis=-1, keepdims=True)
    normed = (centered * lax.rsqrt(variance + EPSILON) * gain_ref[...]).astype(BF)
    normed_ref[...] = normed
    for t in range(3):
        qkv_ref[t] = dot_nn(normed, w_ref[:, features * t : features * (t + 1)]).astype(BF)
    allow = allow_ref[0] > 0.5
    masks = lane_masks()
    for b in range(count_b):
        rows = slice(b * stride, (b + 1) * stride)
        for pair in range(features // 128):
            lanes = pl.ds(128 * pair, 128)
            q2 = qkv_ref[0, rows, lanes] * jnp.asarray(0.125, BF)
            s2 = dot_nt(stack_heads(qkv_ref[1, rows, lanes], masks), q2)
            probs = []
            for h in range(2):
                s = jnp.where(allow, s2[h * stride : (h + 1) * stride], -1e30)
                e = jnp.exp(s - jnp.max(s, axis=0, keepdims=True))
                probs.append((e * (1.0 / jnp.sum(e, axis=0, keepdims=True))).astype(BF))
            p2 = jnp.concatenate(probs, axis=0)
            prob_ref[pair, pl.ds(2 * stride * b, 2 * stride), :] = p2
            win_ref[rows, lanes] = dot_tn(p2, stack_heads(qkv_ref[2, rows, lanes], masks))
    write_edges(unload_windows(win_ref, grid_ref, stride), att_ref, lon_ref, lat_ref, corner_out_ref)


def write_edges(values, out_ref, lon_ref, lat_ref, corner_ref):
    cols = values.shape[0] // WLAT
    out_ref[...] = values.astype(out_ref.dtype)
    edge = jnp.concatenate([values[r * cols : r * cols + EDGE] for r in range(WLAT)], axis=0).astype(BF)
    lon_ref[...] = edge

    @pl.when(pl.program_id(0) == 0)
    def _():
        lat_ref[...] = values[: lat_ref.shape[0]].astype(BF)
        corner_ref[...] = edge[: corner_ref.shape[0]]


def assemble_kernel(stride, own_ref, west_ref, south_ref, corner_ref, out_ref, buf_ref, win_ref):
    load_windows(own_ref, west_ref, south_ref, corner_ref, buf_ref, win_ref, stride)
    out_ref[...] = win_ref[...].astype(BF)


def middle_kernel(cols, tok_ref, att_ref, w_out_ref, gain_ref, grad_in_ref, to_patch_ref,
                  from_patch_ref, merged_in_ref, grad_mixed_ref, grad_att_ref, lon_ref, lat_ref,
                  corner_ref):
    tokens, features = tok_ref.shape
    pairs = tokens // (2 * cols)
    half = cols // 2
    mixed = (tok_ref[...].astype(F32) + dot_nn(att_ref[...], w_out_ref[...])).astype(BF)
    parts = [dot_nn(to_patch_ref[...], mixed[2 * cols * i : 2 * cols * (i + 1)]) for i in range(pairs)]
    groups = [
        jnp.concatenate([part[half * g : half * (g + 1)] for part in parts], axis=0) for g in range(4)
    ]
    width = 4 * features
    average = sum(jnp.sum(v, axis=-1, keepdims=True) for v in groups) / width
    groups = [v - average for v in groups]
    variance = sum(jnp.sum(v * v, axis=-1, keepdims=True) for v in groups) / width
    inv = lax.rsqrt(variance + EPSILON)
    groups = [v * inv for v in groups]
    grads = []
    for g in range(4):
        span = slice(features * g, features * (g + 1))
        gain = gain_ref[:, span]
        merged_in_ref[:, span] = (groups[g] * gain).astype(BF)
        grads.append(grad_in_ref[:, span].astype(F32) * gain)
    mean_one = sum(jnp.sum(v, axis=-1, keepdims=True) for v in grads) / width
    mean_two = sum(
        jnp.sum(v * h, axis=-1, keepdims=True) for v, h in zip(grads, groups)
    ) / width
    outs = [(v - mean_one - h * mean_two) * inv for v, h in zip(grads, groups)]
    for i in range(pairs):
        piece = jnp.concatenate([v[half * i : half * (i + 1)] for v in outs], axis=0).astype(BF)
        back = dot_nn(from_patch_ref[...], piece).astype(BF)
        grad_mixed_ref[pl.ds(2 * cols * i, 2 * cols), :] = back
    grad_att = dot_nt(grad_mixed_ref[...], w_out_ref[...])
    grad_att_ref[...] = grad_att.astype(BF)
    edge = [grad_att[r * cols - EDGE : r * cols] for r in range(1, tokens // cols + 1)]
    lon_ref[...] = jnp.concatenate(edge, axis=0).astype(BF)

    @pl.when(pl.program_id(0) == pl.num_programs(0) - 1)
    def _():
        lat_ref[...] = grad_att[tokens - lat_ref.shape[0] :].astype(BF)
        corner_ref[...] = jnp.concatenate(edge[-(WLAT // 2) :], axis=0).astype(BF)


def grad_in_kernel(gm_ref, w_merge_ref, out_ref):
    out_ref[...] = dot_nt(gm_ref[...], w_merge_ref[...]).astype(BF)


def merge_grad_kernel(merged_in_ref, gm_ref, att_ref, gmix_ref, out_ref):
    width = gm_ref.shape[1]
    out_ref[:, :width] = dot_tn(merged_in_ref[...], gm_ref[...]).astype(BF)
    out_ref[:, width:] = dot_tn(gmix_ref[...], att_ref[...]).T.astype(BF)


def row_sums(value):
    total = sum(value[:, 128 * k : 128 * (k + 1)] for k in range(value.shape[1] // 128))
    return jnp.sum(total.T, axis=0, keepdims=True)


def merge_last_kernel(half, keep_ref, own_ref, got_ref, w_ref, gain_ref, out_ref, out_o_ref, dgain_ref):
    width = w_ref.shape[1]
    here = pl.program_id(0) // half == keep_ref[0]

    def finish(ref):
        value = ref[:, :width].astype(F32)
        out_ref[...] = value
        out_o_ref[...] = ref[:, width:].astype(F32)
        dgain_ref[...] = row_sums(value * w_ref[...].astype(F32)) / gain_ref[...]

    @pl.when(here)
    def _():
        finish(own_ref)

    @pl.when(jnp.logical_not(here))
    def _():
        finish(got_ref)


def qkv_last_kernel(half, keep_ref, own_ref, got_ref, w_ref, gain_ref, out_ref, dgain_ref):
    step = pl.program_id(0)
    here = step // half == keep_ref[0]
    side = pl.ds(step % 2, 1)

    def finish(ref):
        value = ref[...].astype(F32)
        out_ref[...] = value
        part = row_sums(value * w_ref[...].astype(F32))

        @pl.when(step < 2)
        def _():
            dgain_ref[side, :] = part / gain_ref[side, :]

        @pl.when(step >= 2)
        def _():
            dgain_ref[side, :] += part / gain_ref[side, :]

    @pl.when(here)
    def _():
        finish(own_ref)

    @pl.when(jnp.logical_not(here))
    def _():
        finish(got_ref)


def backward_kernel(stride, count_b, ga_ref, qkv_ref, prob_ref, prev_ref, gqkv_ref):
    del prev_ref
    masks = lane_masks()
    low = lax.broadcasted_iota(jnp.int32, (1, 128), 1) < 64
    spans = [slice(b * stride, (b + 1) * stride) for b in range(count_b)]
    for pair in range(ga_ref.shape[1] // 128):
        lanes = pl.ds(128 * pair, 128)
        work = []
        for b, rows in enumerate(spans):
            do2 = ga_ref[rows, lanes]
            p2 = prob_ref[pair, pl.ds(2 * stride * b, 2 * stride), :]
            dp2 = dot_nt(stack_heads(qkv_ref[2, rows, lanes], masks), do2)
            dv = dot_nn(p2, do2)
            gqkv_ref[2, rows, lanes] = jnp.where(low, dv[:stride], dv[stride:]).astype(BF)
            work.append((p2, dp2))
        scores = []
        for p2, dp2 in work:
            grads = []
            for h in range(2):
                p = p2[h * stride : (h + 1) * stride].astype(F32)
                dp = dp2[h * stride : (h + 1) * stride]
                grads.append((p * (dp - jnp.sum(dp * p, axis=0, keepdims=True))).astype(BF))
            scores.append(jnp.concatenate(grads, axis=0))
        for rows, ds2 in zip(spans, scores):
            q2 = qkv_ref[0, rows, lanes] * jnp.asarray(0.125, BF)
            dk = dot_nn(ds2, q2)
            dq = dot_tn(ds2, stack_heads(qkv_ref[1, rows, lanes], masks))
            gqkv_ref[0, rows, lanes] = (dq * 0.125).astype(BF)
            gqkv_ref[1, rows, lanes] = jnp.where(low, dk[:stride], dk[stride:]).astype(BF)


def qkv_grad_kernel(normed_ref, gqkv_ref, out_ref):
    for t in range(3):
        out_ref[t] = dot_tn(normed_ref[...], gqkv_ref[t]).astype(BF)


def input_grad_kernel(stride, gqkv_ref, x_ref, gain_ref, w_ref, out_ref, lon_ref, lat_ref, corner_ref,
                      win_ref, grid_ref):
    features = x_ref.shape[1]
    grad = sum(dot_nt(gqkv_ref[t], w_ref[:, features * t : features * (t + 1)]) for t in range(3))
    x = x_ref[...].astype(F32)
    centered = x - jnp.mean(x, axis=-1, keepdims=True)
    inv = lax.rsqrt(jnp.mean(centered * centered, axis=-1, keepdims=True) + EPSILON)
    hat = centered * inv
    grad = grad * gain_ref[...]
    one = jnp.mean(grad, axis=-1, keepdims=True)
    two = jnp.mean(grad * hat, axis=-1, keepdims=True)
    win_ref[...] = (grad - one - hat * two) * inv
    write_edges(unload_windows(win_ref, grid_ref, stride), out_ref, lon_ref, lat_ref, corner_ref)


def merged_kernel(a_ref, w_ref, out_ref):
    out_ref[...] = dot_nn(a_ref[...], w_ref[...]).astype(BF)


def whole(shape):
    return pl.BlockSpec(shape, lambda i: (0,) * len(shape))


def rows_of(height, width):
    return pl.BlockSpec((height, width), lambda i: (i, 0))


def shift_pairs(count_lat, count_lon, dlat, dlon):
    return [
        (a * count_lon + b, ((a + dlat) % count_lat) * count_lon + (b + dlon) % count_lon)
        for a in range(count_lat)
        for b in range(count_lon)
    ]


def send(value, dlat, dlon):
    pairs = shift_pairs(lax.axis_size("lat"), lax.axis_size("lon"), dlat, dlon)
    return lax.ppermute(value, ("lat", "lon"), pairs)


def exchange(parts, sign):
    lon_edge, lat_edge, corner = parts
    lon_edge = send(lon_edge, 0, sign)
    lat_edge = send(lat_edge, sign, 0)
    corner = send(corner, sign, sign)
    return lon_edge, lat_edge, corner


def edges(values):
    rows, cols, features = values.shape
    hr = WLAT // 2
    parts = (values[:, cols - EDGE :], values[rows - hr :], values[rows - hr :, cols - EDGE :])
    return [v.reshape(-1, features) for v in parts]


def to_own(values, parts):
    rows, cols, features = values.shape
    hr, hc = WLAT // 2, WLON // 2
    east, north, corner = (v.astype(values.dtype) for v in parts)
    top = jnp.concatenate([values[hr:, hc:], east.reshape(rows, EDGE, features)[hr:, :hc]], axis=1)
    north = north.reshape(hr, cols, features)[:, hc:]
    bottom = jnp.concatenate([north, corner.reshape(hr, EDGE, features)[:, :hc]], axis=1)
    return jnp.concatenate([top, bottom], axis=0)


def part_sum(terms, index, height):
    parts = [lax.dynamic_slice_in_dim(t, index * height, height, 0).astype(F32) for t in terms]
    return sum(parts[1:], parts[0]).astype(BF)


def join(value, received, keep):
    first = jnp.where(keep == 0, value, received)
    second = jnp.where(keep == 0, received, value)
    return jnp.concatenate([first, second], axis=0)


def reduce_all(value):
    count_lat, count_lon = lax.axis_size("lat"), lax.axis_size("lon")
    bits = count_lon.bit_length() - 1
    me, lat = lax.axis_index("lon"), lax.axis_index("lat")
    odd = lax.rem(me, 2)
    plans = [([(i, i ^ 1) for i in range(count_lon)], odd)]
    for k in range(bits - 1):
        low, high = 2 << k, 2 << (bits - 2 - k)
        pairs = [(i, i ^ (low if i % 2 == 0 else high)) for i in range(count_lon)]
        keep = jnp.where(odd == 0, lax.rem(me // low, 2), lax.rem(me // high, 2))
        plans.append((pairs, keep))
    terms, height = [value], value.shape[0]
    for pairs, keep in plans:
        height = height // 2
        sent = part_sum(terms, 1 - keep, height)
        received = lax.ppermute(sent, "lon", pairs)
        terms = [lax.dynamic_slice_in_dim(t, keep * height, height, 0) for t in terms] + [received]
    height = height // count_lat
    total = [lax.dynamic_slice_in_dim(t, lat * height, height, 0).astype(F32) for t in terms]
    for d in range(1, count_lat):
        sent = part_sum(terms, lat ^ d, height)
        received = lax.ppermute(sent, "lat", [(i, i ^ d) for i in range(count_lat)])
        total.append(received.astype(F32))
    mine = sum(total[1:], total[0]).astype(BF)
    value = jnp.zeros((count_lat * height,) + mine.shape[1:], BF)
    value = lax.dynamic_update_slice_in_dim(value, mine, lat * height, 0)
    for d in range(1, count_lat):
        received = lax.ppermute(mine, "lat", [(i, i ^ d) for i in range(count_lat)])
        value = lax.dynamic_update_slice_in_dim(value, received, (lat ^ d) * height, 0)
    for k, (pairs, keep) in reversed(list(enumerate(plans))):
        received = lax.ppermute(value, "lon", pairs)
        if k:
            value = join(value, received, keep)
    return value, received, odd.astype(jnp.int32).reshape(1)


def on_device_body(tokens, lat_band, gain_attn, w_qkv, w_out, gain_merge, w_merge, grad_merged):
    rows, cols, features = tokens.shape
    width2 = grad_merged.shape[2]
    count_a, count_b = rows // WLAT, cols // WLON
    window = WLAT * WLON
    stride = -(-window // 16) * 16
    half_lat = WLAT // 2
    block = WLAT * cols
    wide = WLAT * (cols + EDGE)
    padded = count_b * stride
    total = rows * cols
    patch_np = patch_matrix(cols)
    to_patch = jnp.asarray(patch_np, BF)
    from_patch = jnp.asarray(patch_np.T, BF)

    band_count = lat_band.shape[0]
    extended = jnp.concatenate([lat_band[band_count - half_lat :], lat_band])
    band_rows = lax.dynamic_slice_in_dim(extended, lax.axis_index("lat") * rows, rows)
    labels = jnp.repeat(band_rows.reshape(count_a, WLAT), WLON, axis=1)
    labels = jnp.pad(labels, ((0, 0), (0, stride - window)), constant_values=-1)
    allow = (labels[:, :, None] == labels[:, None, :]).astype(F32)
    gain_a = gain_attn.reshape(1, features)
    gain_m = gain_merge.reshape(1, 4 * features)

    own_tok = tokens.reshape(total, features)
    edge_shapes = [(rows * EDGE, features), (half_lat * cols, features), (half_lat * EDGE, features)]
    edge_types = [jax.ShapeDtypeStruct(shape, BF) for shape in edge_shapes]
    edge_specs = [rows_of(WLAT * EDGE, features), whole(edge_shapes[1]), whole(edge_shapes[2])]
    halo_specs = [whole((total, features)), whole((rows, EDGE, features)), whole(edge_shapes[1]),
                  whole((half_lat, EDGE, features))]
    win_scratch = pltpu.VMEM((padded, features), F32)
    buf_scratch = pltpu.VMEM((wide, features), F32)
    grid_scratch = pltpu.VMEM((block, features), F32)

    def halo_args(parts):
        west, south, corner = parts
        return west.reshape(rows, EDGE, features), south, corner.reshape(half_lat, EDGE, features)

    tok_halos = exchange(edges(tokens), 1)
    allow_spec = pl.BlockSpec((1, stride, stride), lambda i: (i, 0, 0))
    pairs = features // 128
    tall3 = count_a * padded
    qkv_spec = pl.BlockSpec((3, padded, features), lambda i: (0, i, 0))
    prob_rows = 2 * stride * count_b
    attended, qkv, normed, tok_win, probs, *att_edges = pl.pallas_call(
        functools.partial(forward_kernel, stride, count_b),
        grid=(count_a,),
        in_specs=halo_specs + [allow_spec, whole((1, features)), whole((features, 3 * features))],
        out_specs=[rows_of(block, features), qkv_spec, rows_of(padded, features),
                   rows_of(padded, features),
                   pl.BlockSpec((pairs, prob_rows, stride), lambda i: (0, i, 0))] + edge_specs,
        out_shape=[jax.ShapeDtypeStruct((total, features), BF),
                   jax.ShapeDtypeStruct((3, tall3, features), BF),
                   jax.ShapeDtypeStruct((tall3, features), BF),
                   jax.ShapeDtypeStruct((tall3, features), BF),
                   jax.ShapeDtypeStruct((pairs, count_a * prob_rows, stride), BF)] + edge_types,
        scratch_shapes=[buf_scratch, win_scratch, grid_scratch],
        compiler_params=params(1),
        cost_estimate=cost(4 * total * features * 3 * features, 2 * total * features * 8),
        name="attn_fwd",
    )(own_tok, *halo_args(tok_halos), allow, gain_a, w_qkv)

    att_parts = exchange(att_edges, -1)
    own_att = to_own(attended.reshape(rows, cols, features), att_parts).reshape(total, features)
    gm = grad_merged.reshape(total // 4, width2)
    grad_in = pl.pallas_call(
        grad_in_kernel,
        grid=(4,),
        in_specs=[whole((total // 4, width2)), rows_of(features, width2)],
        out_specs=pl.BlockSpec((total // 4, features), lambda i: (0, i)),
        out_shape=jax.ShapeDtypeStruct((total // 4, 4 * features), BF),
        compiler_params=params(1),
        cost_estimate=cost(2 * total * features * width2, 2 * total * features * 4),
        name="grad_in",
    )(gm, w_merge)

    steps = 2
    tall = total // steps
    short = tall // 4
    merged_in, grad_mixed, grad_att, *grad_edges = pl.pallas_call(
        functools.partial(middle_kernel, cols),
        grid=(steps,),
        in_specs=[rows_of(tall, features), rows_of(tall, features), whole((features, features)),
                  whole((1, 4 * features)), rows_of(short, 4 * features),
                  whole((2 * cols, 2 * cols)), whole((2 * cols, 2 * cols))],
        out_specs=[rows_of(short, 4 * features), rows_of(tall, features), rows_of(tall, features),
                   rows_of(edge_shapes[0][0] // steps, features)] + edge_specs[1:],
        out_shape=[jax.ShapeDtypeStruct((total // 4, 4 * features), BF),
                   jax.ShapeDtypeStruct((total, features), BF),
                   jax.ShapeDtypeStruct((total, features), BF)] + edge_types,
        compiler_params=params(1),
        cost_estimate=cost(8 * total * features * features, 2 * total * features * 6),
        name="merge_mid",
    )(own_tok, own_att, w_out, gain_m, grad_in, to_patch, from_patch)

    att_halos = exchange(grad_edges, 1)
    pieces = 4
    rest = features // pieces
    dw_merge = pl.pallas_call(
        merge_grad_kernel,
        grid=(pieces,),
        in_specs=[pl.BlockSpec((total // 4, features), lambda i: (0, i)),
                  whole((total // 4, width2)), whole((total, features)),
                  pl.BlockSpec((total, rest), lambda i: (0, i))],
        out_specs=rows_of(features, width2 + rest),
        out_shape=jax.ShapeDtypeStruct((pieces * features, width2 + rest), BF),
        compiler_params=params(1),
        cost_estimate=cost(4 * total * features * features * 2, 2 * total * features * 6),
        name="merge_dw",
    )(merged_in, gm, own_att, grad_mixed)
    sum_m = reduce_all(dw_merge)

    grad_win = pl.pallas_call(
        functools.partial(assemble_kernel, stride),
        grid=(count_a,),
        in_specs=halo_specs,
        out_specs=rows_of(padded, features),
        out_shape=jax.ShapeDtypeStruct((tall3, features), BF),
        scratch_shapes=[buf_scratch, win_scratch],
        compiler_params=params(1),
        cost_estimate=cost(total * features * 1200, 2 * total * features * 3),
        name="assemble",
    )(grad_att, *halo_args(att_halos))
    calls = CALLS
    wide = features // calls
    grad_qkv = None
    for j in range(calls):
        spec = pl.BlockSpec((3, padded, wide), lambda i, j=j: (0, i, j))
        operands = [grad_win, qkv, probs]
        specs = [pl.BlockSpec((padded, wide), lambda i, j=j: (i, j)), spec,
                 pl.BlockSpec((pairs // calls, prob_rows, stride), lambda i, j=j: (j, i, 0))]
        if grad_qkv is not None:
            operands.append(grad_qkv)
            specs.append(pl.BlockSpec(memory_space=pl.ANY))
            body = functools.partial(backward_kernel, stride, count_b)
        else:
            def body(ga_ref, qkv_ref, prob_ref, gqkv_ref):
                backward_kernel(stride, count_b, ga_ref, qkv_ref, prob_ref, None, gqkv_ref)
        grad_qkv = pl.pallas_call(
            body,
            grid=(count_a,),
            in_specs=specs,
            out_specs=spec,
            out_shape=jax.ShapeDtypeStruct((3, tall3, features), BF),
            input_output_aliases={3: 0} if j else {},
            compiler_params=params(1),
            cost_estimate=cost(4 * total * features * 3 * features // calls,
                               2 * total * features * 8 // calls),
        )(*operands)
    dw_q = pl.pallas_call(
        qkv_grad_kernel,
        grid=(2,),
        in_specs=[pl.BlockSpec((tall3, features // 2), lambda i: (0, i)),
                  whole((3, tall3, features))],
        out_specs=pl.BlockSpec((3, features // 2, features), lambda i: (0, i, 0)),
        out_shape=jax.ShapeDtypeStruct((3, features, features), BF),
        compiler_params=params(1),
        cost_estimate=cost(2 * total * features * 3 * features, 2 * total * features * 5),
        name="qkv_dw",
    )(normed, grad_qkv)
    sum_q = reduce_all(dw_q.reshape(3 * features, features))

    grad_inputs, *in_edges = pl.pallas_call(
        functools.partial(input_grad_kernel, stride),
        grid=(count_a,),
        in_specs=[qkv_spec, rows_of(padded, features), whole((1, features)),
                  whole((features, 3 * features))],
        out_specs=[rows_of(block, features)] + edge_specs,
        out_shape=[jax.ShapeDtypeStruct((total, features), BF)] + edge_types,
        scratch_shapes=[win_scratch, grid_scratch],
        compiler_params=params(1),
        cost_estimate=cost(2 * total * features * 3 * features, 2 * total * features * 6),
        name="input_grad",
    )(grad_qkv, tok_win, gain_a, w_qkv)
    in_parts = exchange(in_edges, -1)
    grad_own = to_own(grad_inputs.reshape(rows, cols, features), in_parts)
    grad_tokens = grad_own.astype(F32) + grad_mixed.reshape(rows, cols, features).astype(F32)

    merged = pl.pallas_call(
        merged_kernel,
        grid=(2,),
        in_specs=[rows_of(total // 8, 4 * features), whole((4 * features, width2))],
        out_specs=rows_of(total // 8, width2),
        out_shape=jax.ShapeDtypeStruct((total // 4, width2), BF),
        compiler_params=params(1),
        cost_estimate=cost(2 * total * features * width2, 2 * total * features * 4),
        name="merged",
    )(merged_in, w_merge).reshape(grad_merged.shape)

    def halves(height, width, half):
        def spot(mine):
            def index(i, keep):
                side, place = i // half, i % half
                other = jnp.where(side < (keep[0] if mine else 1 - keep[0]), 0, half - 1)
                return jnp.where((side == keep[0]) == mine, place, other), 0

            return index

        return [pl.BlockSpec((height, width), spot(True)), pl.BlockSpec((height, width), spot(False))]

    m_own, m_got, keep = sum_m
    grad_w_merge, grad_w_out, grad_gain_merge = pl.pallas_call(
        functools.partial(merge_last_kernel, pieces // 2),
        grid_spec=pltpu.PrefetchScalarGridSpec(
            num_scalar_prefetch=1,
            grid=(pieces,),
            in_specs=halves(features, width2 + rest, pieces // 2) + [
                pl.BlockSpec((features, width2), lambda i, k: (i, 0)),
                pl.BlockSpec((1, features), lambda i, k: (0, i))],
            out_specs=[pl.BlockSpec((features, width2), lambda i, k: (i, 0)),
                       pl.BlockSpec((features, rest), lambda i, k: (0, i)),
                       pl.BlockSpec((1, features), lambda i, k: (0, i))],
        ),
        out_shape=[jax.ShapeDtypeStruct((pieces * features, width2), F32),
                   jax.ShapeDtypeStruct((features, features), F32),
                   jax.ShapeDtypeStruct((1, pieces * features), F32)],
        compiler_params=params(1),
        cost_estimate=cost(total * features * 2000, 2 * total * features * 6),
        name="m_last",
    )(keep, m_own, m_got, w_merge, gain_m)
    q_own, q_got, keep = sum_q
    tile = features // 2
    grad_w_qkv, grad_gain_attn = pl.pallas_call(
        functools.partial(qkv_last_kernel, 3),
        grid_spec=pltpu.PrefetchScalarGridSpec(
            num_scalar_prefetch=1,
            grid=(6,),
            in_specs=halves(tile, features, 3) + [
                pl.BlockSpec((tile, features), lambda i, k: (i % 2, i // 2)),
                pl.BlockSpec((2, tile), lambda i, k: (0, 0))],
            out_specs=[pl.BlockSpec((tile, features), lambda i, k: (i % 2, i // 2)),
                       pl.BlockSpec((2, tile), lambda i, k: (0, 0))],
        ),
        out_shape=[jax.ShapeDtypeStruct((features, 3 * features), F32),
                   jax.ShapeDtypeStruct((2, tile), F32)],
        compiler_params=params(1),
        cost_estimate=cost(total * features * 1000, 2 * total * features * 3),
        name="q_last",
    )(keep, q_own, q_got, w_qkv, gain_attn.reshape(2, tile))
    grad_gain_merge = grad_gain_merge.reshape(-1)
    grad_gain_attn = grad_gain_attn.reshape(-1)
    return (merged, grad_tokens, grad_gain_attn, grad_w_qkv, grad_w_out, grad_gain_merge,
            grad_w_merge)


def solution(mesh):
    return jax.shard_map(
        on_device_body,
        mesh=mesh,
        in_specs=(P("lat", "lon", None), P(), P(), P(), P(), P(), P(), P("lat", "lon", None)),
        out_specs=(P("lat", "lon", None), P("lat", "lon", None), P(), P(), P(), P(), P()),
        check_vma=False,
    )
```

```python
import functools

import jax
import jax.numpy as jnp
import numpy as np
from jax import lax
from jax.experimental import pallas as pl
from jax.experimental.pallas import tpu as pltpu
from jax.sharding import PartitionSpec as P


WLAT = 6
WLON = 12
EPSILON = 1e-05
EDGE = 8
BF = jnp.bfloat16
F32 = jnp.float32

CALLS = 4


def dot_nn(a, b):
    return lax.dot_general(a, b, (((1,), (0,)), ((), ())), preferred_element_type=F32)


def dot_nt(a, b):
    return lax.dot_general(a, b, (((1,), (1,)), ((), ())), preferred_element_type=F32)


def dot_tn(a, b):
    return lax.dot_general(a, b, (((0,), (0,)), ((), ())), preferred_element_type=F32)


def params(steps):
    return pltpu.CompilerParams(
        dimension_semantics=("arbitrary",) * steps, vmem_limit_bytes=60 * 1024 * 1024
    )


def cost(flops, nbytes):
    return pl.CostEstimate(flops=int(flops), transcendentals=0, bytes_accessed=int(nbytes))


def patch_matrix(cols):
    half = cols // 2
    mat = np.zeros((4 * half, 2 * cols), np.float32)
    for j in range(half):
        for g, (dr, dc) in enumerate(((0, 0), (1, 0), (0, 1), (1, 1))):
            mat[g * half + j, dr * cols + 2 * j + dc] = 1.0
    return mat


def lane_masks():
    lane = lax.broadcasted_iota(jnp.int32, (1, 128), 1)
    even = (lane < 64).astype(F32)
    return even.astype(BF), (1.0 - even).astype(BF)


def load_rows(deep, own_ref, west_ref, south_ref, corner_ref, buf_ref, win_ref, stride):
    tall, wide = win_ref.shape[0] // deep, buf_ref.shape[0] // deep
    for k in range(deep):
        load_windows(pl.program_id(0) * deep + k, k == 0, own_ref, west_ref, south_ref, corner_ref,
                     buf_ref.at[pl.ds(k * wide, wide)], win_ref.at[pl.ds(k * tall, tall)], stride)


def load_windows(step, first, own_ref, west_ref, south_ref, corner_ref, buf_ref, win_ref, stride):
    cols = south_ref.shape[0] // (WLAT // 2)
    wide = EDGE + cols
    half = WLAT // 2

    def put(r, edge, line):
        buf_ref[pl.ds(wide * r, EDGE), :] = edge.astype(F32)
        buf_ref[pl.ds(wide * r + EDGE, cols), :] = line.astype(F32)

    def later(r):
        row = WLAT * step - half + r
        put(r, west_ref[row], own_ref[pl.ds(pl.multiple_of(cols * row, 16), cols), :])

    if first:
        @pl.when(step == 0)
        def _():
            for r in range(half):
                put(r, corner_ref[r], south_ref[pl.ds(cols * r, cols), :])

        @pl.when(step > 0)
        def _():
            for r in range(half):
                later(r)

    for r in range(0 if not first else half, WLAT):
        later(r)
    for b in range(cols // WLON):
        for r in range(WLAT):
            piece = buf_ref[pl.ds(wide * r + EDGE - WLON // 2 + WLON * b, WLON), :]
            win_ref[pl.ds(stride * b + WLON * r, WLON), :] = piece
        pad = stride - WLAT * WLON
        win_ref[pl.ds(stride * (b + 1) - pad, pad), :] = jnp.zeros((pad, win_ref.shape[1]), F32)


def unload_rows(deep, win_ref, grid_ref, stride, out_ref, lon_ref, lat_ref, corner_ref):
    tall, block = win_ref.shape[0] // deep, grid_ref.shape[0] // deep
    cols = block // WLAT
    for k in range(deep):
        for b in range(cols // WLON):
            for r in range(WLAT):
                piece = win_ref[pl.ds(k * tall + stride * b + WLON * r, WLON), :]
                grid_ref[pl.ds(k * block + cols * r + WLON * b, WLON), :] = piece
    out_ref[...] = grid_ref[...].astype(out_ref.dtype)
    edge = [grid_ref[pl.ds(r * cols, EDGE), :] for r in range(deep * WLAT)]
    edge = jnp.concatenate(edge, axis=0).astype(BF)
    lon_ref[...] = edge

    @pl.when(pl.program_id(0) == 0)
    def _():
        lat_ref[...] = grid_ref[pl.ds(0, lat_ref.shape[0]), :].astype(BF)
        corner_ref[...] = edge[: corner_ref.shape[0]]


def stack_heads(value, masks):
    return jnp.concatenate([value * masks[0], value * masks[1]], axis=0)


def forward_kernel(deep, stride, count_b, own_ref, west_ref, south_ref, corner_ref, allow_ref, gain_ref,
                   w_ref, att_ref, qkv_ref, normed_ref, tok_ref, prob_ref, lon_ref, lat_ref,
                   corner_out_ref, buf_ref, win_ref, grid_ref):
    features = own_ref.shape[1]
    load_rows(deep, own_ref, west_ref, south_ref, corner_ref, buf_ref, win_ref, stride)
    x = win_ref[...]
    tok_ref[...] = x.astype(BF)
    average = jnp.mean(x, axis=-1, keepdims=True)
    centered = x - average
    variance = jnp.mean(centered * centered, axis=-1, keepdims=True)
    normed = (centered * lax.rsqrt(variance + EPSILON) * gain_ref[...]).astype(BF)
    normed_ref[...] = normed
    for t in range(3):
        qkv_ref[t] = dot_nn(normed, w_ref[:, features * t : features * (t + 1)]).astype(BF)
    masks = lane_masks()
    for b in range(deep * count_b):
        allow = allow_ref[b // count_b] > 0.5
        rows = slice(b * stride, (b + 1) * stride)
        for pair in range(features // 128):
            lanes = pl.ds(128 * pair, 128)
            q2 = qkv_ref[0, rows, lanes] * jnp.asarray(0.125, BF)
            s2 = dot_nt(stack_heads(qkv_ref[1, rows, lanes], masks), q2)
            probs = []
            for h in range(2):
                s = jnp.where(allow, s2[h * stride : (h + 1) * stride], -1e30)
                e = jnp.exp(s - jnp.max(s, axis=0, keepdims=True))
                probs.append((e * (1.0 / jnp.sum(e, axis=0, keepdims=True))).astype(BF))
            p2 = jnp.concatenate(probs, axis=0)
            prob_ref[pair, pl.ds(2 * stride * b, 2 * stride), :] = p2
            win_ref[rows, lanes] = dot_tn(p2, stack_heads(qkv_ref[2, rows, lanes], masks))
    unload_rows(deep, win_ref, grid_ref, stride, att_ref, lon_ref, lat_ref, corner_out_ref)


def assemble_kernel(deep, stride, own_ref, west_ref, south_ref, corner_ref, out_ref, buf_ref, win_ref):
    load_rows(deep, own_ref, west_ref, south_ref, corner_ref, buf_ref, win_ref, stride)
    out_ref[...] = win_ref[...].astype(BF)


def middle_kernel(cols, tok_ref, att_ref, w_out_ref, gain_ref, grad_in_ref, to_patch_ref,
                  from_patch_ref, merged_in_ref, grad_mixed_ref, grad_att_ref, lon_ref, lat_ref,
                  corner_ref):
    tokens, features = tok_ref.shape
    pairs = tokens // (2 * cols)
    half = cols // 2
    mixed = (tok_ref[...].astype(F32) + dot_nn(att_ref[...], w_out_ref[...])).astype(BF)
    parts = [dot_nn(to_patch_ref[...], mixed[2 * cols * i : 2 * cols * (i + 1)]) for i in range(pairs)]
    groups = [
        jnp.concatenate([part[half * g : half * (g + 1)] for part in parts], axis=0) for g in range(4)
    ]
    width = 4 * features
    average = sum(jnp.sum(v, axis=-1, keepdims=True) for v in groups) / width
    groups = [v - average for v in groups]
    variance = sum(jnp.sum(v * v, axis=-1, keepdims=True) for v in groups) / width
    inv = lax.rsqrt(variance + EPSILON)
    groups = [v * inv for v in groups]
    grads = []
    for g in range(4):
        span = slice(features * g, features * (g + 1))
        gain = gain_ref[:, span]
        merged_in_ref[:, span] = (groups[g] * gain).astype(BF)
        grads.append(grad_in_ref[:, span].astype(F32) * gain)
    mean_one = sum(jnp.sum(v, axis=-1, keepdims=True) for v in grads) / width
    mean_two = sum(
        jnp.sum(v * h, axis=-1, keepdims=True) for v, h in zip(grads, groups)
    ) / width
    outs = [(v - mean_one - h * mean_two) * inv for v, h in zip(grads, groups)]
    for i in range(pairs):
        piece = jnp.concatenate([v[half * i : half * (i + 1)] for v in outs], axis=0).astype(BF)
        back = dot_nn(from_patch_ref[...], piece).astype(BF)
        grad_mixed_ref[pl.ds(2 * cols * i, 2 * cols), :] = back
    grad_att = dot_nt(grad_mixed_ref[...], w_out_ref[...])
    grad_att_ref[...] = grad_att.astype(BF)
    edge = [grad_att[r * cols - EDGE : r * cols] for r in range(1, tokens // cols + 1)]
    lon_ref[...] = jnp.concatenate(edge, axis=0).astype(BF)

    @pl.when(pl.program_id(0) == pl.num_programs(0) - 1)
    def _():
        lat_ref[...] = grad_att[tokens - lat_ref.shape[0] :].astype(BF)
        corner_ref[...] = jnp.concatenate(edge[-(WLAT // 2) :], axis=0).astype(BF)


def grad_in_kernel(gm_ref, w_merge_ref, out_ref):
    out_ref[...] = dot_nt(gm_ref[...], w_merge_ref[...]).astype(BF)


def merge_grad_kernel(_, merged_in_ref, gm_ref, att_ref, gmix_ref, out_ref):
    width = gm_ref.shape[1]
    out_ref[:, :width] = dot_tn(merged_in_ref[...], gm_ref[...]).astype(BF)
    out_ref[:, width:] = dot_tn(gmix_ref[...], att_ref[...]).T.astype(BF)


def row_sums(value):
    total = sum(value[:, 128 * k : 128 * (k + 1)] for k in range(value.shape[1] // 128))
    return jnp.sum(total.T, axis=0, keepdims=True)


def merge_last_kernel(_, value_ref, w_ref, gain_ref, *refs):
    out_ref, out_o_ref, dgain_ref = refs[-3:]
    width = w_ref.shape[1]
    value = value_ref[:, :width].astype(F32)
    out_ref[...] = value
    out_o_ref[...] = value_ref[:, width:].astype(F32)
    dgain_ref[...] = row_sums(value * w_ref[...].astype(F32)) / gain_ref[...]


def qkv_last_kernel(_, value_ref, w_ref, gain_ref, *refs):
    out_ref, dgain_ref = refs[-2:]
    height, features = value_ref.shape[0] // 3, value_ref.shape[1]
    total = 0.0
    for t in range(3):
        lanes = slice(features * t, features * (t + 1))
        value = value_ref[height * t : height * (t + 1), :].astype(F32)
        out_ref[:, lanes] = value
        total = total + value * w_ref[:, lanes].astype(F32)
    dgain_ref[...] = row_sums(total) / gain_ref[...]


def backward_kernel(stride, count_b, ga_ref, qkv_ref, prob_ref, prev_ref, gqkv_ref):
    del prev_ref
    masks = lane_masks()
    low = lax.broadcasted_iota(jnp.int32, (1, 128), 1) < 64
    spans = [slice(b * stride, (b + 1) * stride) for b in range(count_b)]
    for pair in range(ga_ref.shape[1] // 128):
        lanes = pl.ds(128 * pair, 128)
        work = []
        for b, rows in enumerate(spans):
            do2 = ga_ref[rows, lanes]
            p2 = prob_ref[pair, pl.ds(2 * stride * b, 2 * stride), :]
            dp2 = dot_nt(stack_heads(qkv_ref[2, rows, lanes], masks), do2)
            dv = dot_nn(p2, do2)
            gqkv_ref[2, rows, lanes] = jnp.where(low, dv[:stride], dv[stride:]).astype(BF)
            work.append((p2, dp2))
        scores = []
        for p2, dp2 in work:
            grads = []
            for h in range(2):
                p = p2[h * stride : (h + 1) * stride].astype(F32)
                dp = dp2[h * stride : (h + 1) * stride]
                grads.append((p * (dp - jnp.sum(dp * p, axis=0, keepdims=True))).astype(BF))
            scores.append(jnp.concatenate(grads, axis=0))
        for rows, ds2 in zip(spans, scores):
            q2 = qkv_ref[0, rows, lanes] * jnp.asarray(0.125, BF)
            dk = dot_nn(ds2, q2)
            dq = dot_tn(ds2, stack_heads(qkv_ref[1, rows, lanes], masks))
            gqkv_ref[0, rows, lanes] = (dq * 0.125).astype(BF)
            gqkv_ref[1, rows, lanes] = jnp.where(low, dk[:stride], dk[stride:]).astype(BF)


def qkv_grad_kernel(_, normed_ref, gqkv_ref, out_ref):
    height = normed_ref.shape[1]
    for t in range(3):
        out_ref[height * t : height * (t + 1), :] = dot_tn(normed_ref[...], gqkv_ref[t]).astype(BF)


def input_grad_kernel(deep, stride, gqkv_ref, x_ref, gain_ref, w_ref, out_ref, lon_ref, lat_ref, corner_ref,
                      win_ref, grid_ref):
    features = x_ref.shape[1]
    grad = sum(dot_nt(gqkv_ref[t], w_ref[:, features * t : features * (t + 1)]) for t in range(3))
    x = x_ref[...].astype(F32)
    centered = x - jnp.mean(x, axis=-1, keepdims=True)
    inv = lax.rsqrt(jnp.mean(centered * centered, axis=-1, keepdims=True) + EPSILON)
    hat = centered * inv
    grad = grad * gain_ref[...]
    one = jnp.mean(grad, axis=-1, keepdims=True)
    two = jnp.mean(grad * hat, axis=-1, keepdims=True)
    win_ref[...] = (grad - one - hat * two) * inv
    unload_rows(deep, win_ref, grid_ref, stride, out_ref, lon_ref, lat_ref, corner_ref)


def merged_kernel(a_ref, w_ref, out_ref):
    out_ref[...] = dot_nn(a_ref[...], w_ref[...]).astype(BF)


def whole(shape):
    return pl.BlockSpec(shape, lambda i: (0,) * len(shape))


def rows_of(height, width):
    return pl.BlockSpec((height, width), lambda i: (i, 0))


def shift_pairs(count_lat, count_lon, dlat, dlon):
    return [
        (a * count_lon + b, ((a + dlat) % count_lat) * count_lon + (b + dlon) % count_lon)
        for a in range(count_lat)
        for b in range(count_lon)
    ]


def send(value, dlat, dlon):
    pairs = shift_pairs(lax.axis_size("lat"), lax.axis_size("lon"), dlat, dlon)
    return lax.ppermute(value, ("lat", "lon"), pairs)


def exchange(parts, sign):
    lon_edge, lat_edge, corner = parts
    lon_edge = send(lon_edge, 0, sign)
    lat_edge = send(lat_edge, sign, 0)
    corner = send(corner, sign, sign)
    return lon_edge, lat_edge, corner


def edges(values):
    rows, cols, features = values.shape
    hr = WLAT // 2
    parts = (values[:, cols - EDGE :], values[rows - hr :], values[rows - hr :, cols - EDGE :])
    return [v.reshape(-1, features) for v in parts]


def to_own(values, parts):
    rows, cols, features = values.shape
    hr, hc = WLAT // 2, WLON // 2
    east, north, corner = (v.astype(values.dtype) for v in parts)
    top = jnp.concatenate([values[hr:, hc:], east.reshape(rows, EDGE, features)[hr:, :hc]], axis=1)
    north = north.reshape(hr, cols, features)[:, hc:]
    bottom = jnp.concatenate([north, corner.reshape(hr, EDGE, features)[:, :hc]], axis=1)
    return jnp.concatenate([top, bottom], axis=0)


def part_sum(terms, index, height):
    parts = [lax.dynamic_slice_in_dim(t, index * height, height, 0).astype(F32) for t in terms]
    return sum(parts[1:], parts[0]).astype(BF)


def join(value, received, keep):
    first = jnp.where(keep == 0, value, received)
    second = jnp.where(keep == 0, received, value)
    return jnp.concatenate([first, second], axis=0)


def reduce_all(sent, kept):
    count_lat, count_lon = lax.axis_size("lat"), lax.axis_size("lon")
    bits = count_lon.bit_length() - 1
    me, lat = lax.axis_index("lon"), lax.axis_index("lat")
    odd = lax.rem(me, 2)
    partner = [(i, i ^ 1) for i in range(count_lon)]
    plans = []
    for k in range(bits - 1):
        low, high = 2 << k, 2 << (bits - 2 - k)
        pairs = [(i, i ^ (low if i % 2 == 0 else high)) for i in range(count_lon)]
        keep = jnp.where(odd == 0, lax.rem(me // low, 2), lax.rem(me // high, 2))
        plans.append((pairs, keep))
    received = lax.ppermute(sent, "lon", partner)
    terms, height = [kept, received], kept.shape[0]
    for k, (pairs, keep) in enumerate(plans, 1):
        height = height // 2
        sent = part_sum(terms, 1 - keep, height)
        received = lax.ppermute(sent, "lon", pairs)
        terms = [lax.dynamic_slice_in_dim(t, keep * height, height, 0) for t in terms] + [received]
    height = height // count_lat
    total = [lax.dynamic_slice_in_dim(t, lat * height, height, 0).astype(F32) for t in terms]
    for d in range(1, count_lat):
        sent = part_sum(terms, lat ^ d, height)
        received = lax.ppermute(sent, "lat", [(i, i ^ d) for i in range(count_lat)])
        total.append(received.astype(F32))
    mine = sum(total[1:], total[0]).astype(BF)
    value = jnp.zeros((count_lat * height,) + mine.shape[1:], BF)
    value = lax.dynamic_update_slice_in_dim(value, mine, lat * height, 0)
    for d in range(1, count_lat):
        received = lax.ppermute(mine, "lat", [(i, i ^ d) for i in range(count_lat)])
        value = lax.dynamic_update_slice_in_dim(value, received, (lat ^ d) * height, 0)
    for k, (pairs, keep) in reversed(list(enumerate(plans, 1))):
        received = lax.ppermute(value, "lon", pairs)
        value = join(value, received, keep)
    received = lax.ppermute(value, "lon", partner)
    return value, received


def on_device_body(tokens, lat_band, gain_attn, w_qkv, w_out, gain_merge, w_merge, grad_merged):
    rows, cols, features = tokens.shape
    width2 = grad_merged.shape[2]
    count_a, count_b = rows // WLAT, cols // WLON
    window = WLAT * WLON
    stride = -(-window // 16) * 16
    half_lat = WLAT // 2
    block = WLAT * cols
    wide = WLAT * (cols + EDGE)
    padded = count_b * stride
    total = rows * cols
    patch_np = patch_matrix(cols)
    to_patch = jnp.asarray(patch_np, BF)
    from_patch = jnp.asarray(patch_np.T, BF)

    band_count = lat_band.shape[0]
    extended = jnp.concatenate([lat_band[band_count - half_lat :], lat_band])
    band_rows = lax.dynamic_slice_in_dim(extended, lax.axis_index("lat") * rows, rows)
    labels = jnp.repeat(band_rows.reshape(count_a, WLAT), WLON, axis=1)
    labels = jnp.pad(labels, ((0, 0), (0, stride - window)), constant_values=-1)
    allow = (labels[:, :, None] == labels[:, None, :]).astype(F32)
    gain_a = gain_attn.reshape(1, features)
    gain_m = gain_merge.reshape(1, 4 * features)

    own_tok = tokens.reshape(total, features)
    edge_shapes = [(rows * EDGE, features), (half_lat * cols, features), (half_lat * EDGE, features)]
    edge_types = [jax.ShapeDtypeStruct(shape, BF) for shape in edge_shapes]
    deep = 2 if count_a % 2 == 0 else 1
    edge_specs = [rows_of(deep * WLAT * EDGE, features), whole(edge_shapes[1]), whole(edge_shapes[2])]
    halo_specs = [whole((total, features)), whole((rows, EDGE, features)), whole(edge_shapes[1]),
                  whole((half_lat, EDGE, features))]
    win_scratch = pltpu.VMEM((deep * padded, features), F32)
    buf_scratch = pltpu.VMEM((deep * wide, features), F32)
    grid_scratch = pltpu.VMEM((deep * block, features), F32)

    def halo_args(parts):
        west, south, corner = parts
        return west.reshape(rows, EDGE, features), south, corner.reshape(half_lat, EDGE, features)

    tok_halos = exchange(edges(tokens), 1)
    allow_spec = pl.BlockSpec((deep, stride, stride), lambda i: (i, 0, 0))
    pairs = features // 128
    tall3 = count_a * padded
    qkv_spec = pl.BlockSpec((3, deep * padded, features), lambda i: (0, i, 0))
    prob_rows = 2 * stride * count_b
    attended, qkv, normed, tok_win, probs, *att_edges = pl.pallas_call(
        functools.partial(forward_kernel, deep, stride, count_b),
        grid=(count_a // deep,),
        in_specs=halo_specs + [allow_spec, whole((1, features)), whole((features, 3 * features))],
        out_specs=[rows_of(deep * block, features), qkv_spec, rows_of(deep * padded, features),
                   rows_of(deep * padded, features),
                   pl.BlockSpec((pairs, deep * prob_rows, stride), lambda i: (0, i, 0))] + edge_specs,
        out_shape=[jax.ShapeDtypeStruct((total, features), BF),
                   jax.ShapeDtypeStruct((3, tall3, features), BF),
                   jax.ShapeDtypeStruct((tall3, features), BF),
                   jax.ShapeDtypeStruct((tall3, features), BF),
                   jax.ShapeDtypeStruct((pairs, count_a * prob_rows, stride), BF)] + edge_types,
        scratch_shapes=[buf_scratch, win_scratch, grid_scratch],
        compiler_params=params(1),
        cost_estimate=cost(4 * total * features * 3 * features, 2 * total * features * 8),
        name="attn_fwd",
    )(own_tok, *halo_args(tok_halos), allow, gain_a, w_qkv)

    att_parts = exchange(att_edges, -1)
    own_att = to_own(attended.reshape(rows, cols, features), att_parts).reshape(total, features)
    gm = grad_merged.reshape(total // 4, width2)
    grad_in = pl.pallas_call(
        grad_in_kernel,
        grid=(2,),
        in_specs=[whole((total // 4, width2)), rows_of(2 * features, width2)],
        out_specs=pl.BlockSpec((total // 4, 2 * features), lambda i: (0, i)),
        out_shape=jax.ShapeDtypeStruct((total // 4, 4 * features), BF),
        compiler_params=params(1),
        cost_estimate=cost(2 * total * features * width2, 2 * total * features * 4),
        name="grad_in",
    )(gm, w_merge)

    steps = 2
    tall = total // steps
    short = tall // 4
    merged_in, grad_mixed, grad_att, *grad_edges = pl.pallas_call(
        functools.partial(middle_kernel, cols),
        grid=(steps,),
        in_specs=[rows_of(tall, features), rows_of(tall, features), whole((features, features)),
                  whole((1, 4 * features)), rows_of(short, 4 * features),
                  whole((2 * cols, 2 * cols)), whole((2 * cols, 2 * cols))],
        out_specs=[rows_of(short, 4 * features), rows_of(tall, features), rows_of(tall, features),
                   rows_of(edge_shapes[0][0] // steps, features)] + edge_specs[1:],
        out_shape=[jax.ShapeDtypeStruct((total // 4, 4 * features), BF),
                   jax.ShapeDtypeStruct((total, features), BF),
                   jax.ShapeDtypeStruct((total, features), BF)] + edge_types,
        compiler_params=params(1),
        cost_estimate=cost(8 * total * features * features, 2 * total * features * 6),
        name="merge_mid",
    )(own_tok, own_att, w_out, gain_m, grad_in, to_patch, from_patch)

    att_halos = exchange(grad_edges, 1)
    pieces = 4
    rest = features // pieces
    odd = lax.rem(lax.axis_index("lon"), 2).astype(jnp.int32)
    mine, theirs = odd.reshape(1), (1 - odd).reshape(1)

    def merge_dw(side):
        return pl.pallas_call(
            merge_grad_kernel,
            grid_spec=pltpu.PrefetchScalarGridSpec(
                num_scalar_prefetch=1,
                grid=(pieces // 2,),
                in_specs=[pl.BlockSpec((total // 4, features), lambda i, k: (0, 2 * k[0] + i)),
                          pl.BlockSpec((total // 4, width2), lambda i, k: (0, 0)),
                          pl.BlockSpec((total, features), lambda i, k: (0, 0)),
                          pl.BlockSpec((total, rest), lambda i, k: (0, 2 * k[0] + i))],
                out_specs=pl.BlockSpec((features, width2 + rest), lambda i, k: (i, 0)),
            ),
            out_shape=jax.ShapeDtypeStruct((pieces // 2 * features, width2 + rest), BF),
            compiler_params=params(1),
            cost_estimate=cost(2 * total * features * features * 2, total * features * 6),
            name="merge_dw",
        )(side, merged_in, gm, own_att, grad_mixed)

    m_own, m_got = reduce_all(merge_dw(theirs), merge_dw(mine))

    grad_win = pl.pallas_call(
        functools.partial(assemble_kernel, count_a, stride),
        grid=(1,),
        in_specs=halo_specs,
        out_specs=rows_of(tall3, features),
        out_shape=jax.ShapeDtypeStruct((tall3, features), BF),
        scratch_shapes=[pltpu.VMEM((count_a * wide, features), F32), pltpu.VMEM((tall3, features), F32)],
        compiler_params=params(1),
        cost_estimate=cost(total * features * 1200, 2 * total * features * 3),
        name="assemble",
    )(grad_att, *halo_args(att_halos))
    calls = CALLS
    lane_count = features // calls
    grad_qkv = None
    for j in range(calls):
        spec = pl.BlockSpec((3, deep * padded, lane_count), lambda i, j=j: (0, i, j))
        operands = [grad_win, qkv, probs]
        specs = [pl.BlockSpec((deep * padded, lane_count), lambda i, j=j: (i, j)), spec,
                 pl.BlockSpec((pairs // calls, deep * prob_rows, stride), lambda i, j=j: (j, i, 0))]
        if grad_qkv is not None:
            operands.append(grad_qkv)
            specs.append(pl.BlockSpec(memory_space=pl.ANY))
            body = functools.partial(backward_kernel, stride, deep * count_b)
        else:
            def body(ga_ref, qkv_ref, prob_ref, gqkv_ref):
                backward_kernel(stride, deep * count_b, ga_ref, qkv_ref, prob_ref, None, gqkv_ref)
        grad_qkv = pl.pallas_call(
            body,
            grid=(count_a // deep,),
            in_specs=specs,
            out_specs=spec,
            out_shape=jax.ShapeDtypeStruct((3, tall3, features), BF),
            input_output_aliases={3: 0} if j else {},
            compiler_params=params(1),
            cost_estimate=cost(4 * total * features * 3 * features // calls,
                               2 * total * features * 8 // calls),
        )(*operands)
    tile = features // 2

    def qkv_dw(side):
        return pl.pallas_call(
            qkv_grad_kernel,
            grid_spec=pltpu.PrefetchScalarGridSpec(
                num_scalar_prefetch=1,
                grid=(1,),
                in_specs=[pl.BlockSpec((tall3, tile), lambda i, k: (0, k[0])),
                          pl.BlockSpec((3, tall3, features), lambda i, k: (0, 0, 0))],
                out_specs=pl.BlockSpec((3 * tile, features), lambda i, k: (0, 0)),
            ),
            out_shape=jax.ShapeDtypeStruct((3 * tile, features), BF),
            compiler_params=params(1),
            cost_estimate=cost(total * features * 3 * features, total * features * 5),
            name="qkv_dw",
        )(side, normed, grad_qkv)

    q_own, q_got = reduce_all(qkv_dw(theirs), qkv_dw(mine))

    grad_inputs, *in_edges = pl.pallas_call(
        functools.partial(input_grad_kernel, deep, stride),
        grid=(count_a // deep,),
        in_specs=[qkv_spec, rows_of(deep * padded, features), whole((1, features)),
                  whole((features, 3 * features))],
        out_specs=[rows_of(deep * block, features)] + edge_specs,
        out_shape=[jax.ShapeDtypeStruct((total, features), BF)] + edge_types,
        scratch_shapes=[win_scratch, grid_scratch],
        compiler_params=params(1),
        cost_estimate=cost(2 * total * features * 3 * features, 2 * total * features * 6),
        name="input_grad",
    )(grad_qkv, tok_win, gain_a, w_qkv)
    in_parts = exchange(in_edges, -1)
    grad_own = to_own(grad_inputs.reshape(rows, cols, features), in_parts)
    grad_tokens = grad_own.astype(F32) + grad_mixed.reshape(rows, cols, features).astype(F32)

    merged = pl.pallas_call(
        merged_kernel,
        grid=(2,),
        in_specs=[whole((total // 4, 4 * features)),
                  pl.BlockSpec((4 * features, width2 // 2), lambda i: (0, i))],
        out_specs=pl.BlockSpec((total // 4, width2 // 2), lambda i: (0, i)),
        out_shape=jax.ShapeDtypeStruct((total // 4, width2), BF),
        compiler_params=params(1),
        cost_estimate=cost(2 * total * features * width2, 2 * total * features * 4),
        name="merged",
    )(merged_in, w_merge).reshape(grad_merged.shape)

    def finish_merge(side, value, earlier=()):
        return pl.pallas_call(
            merge_last_kernel,
            grid_spec=pltpu.PrefetchScalarGridSpec(
                num_scalar_prefetch=1,
                grid=(pieces // 2,),
                in_specs=[pl.BlockSpec((features, width2 + rest), lambda i, k: (i, 0)),
                          pl.BlockSpec((features, width2), lambda i, k: (2 * k[0] + i, 0)),
                          pl.BlockSpec((1, features), lambda i, k: (0, 2 * k[0] + i))]
                + [pl.BlockSpec(memory_space=pl.ANY)] * len(earlier),
                out_specs=[pl.BlockSpec((features, width2), lambda i, k: (2 * k[0] + i, 0)),
                           pl.BlockSpec((features, rest), lambda i, k: (0, 2 * k[0] + i)),
                           pl.BlockSpec((1, features), lambda i, k: (0, 2 * k[0] + i))],
            ),
            out_shape=[jax.ShapeDtypeStruct((pieces * features, width2), F32),
                       jax.ShapeDtypeStruct((features, features), F32),
                       jax.ShapeDtypeStruct((1, pieces * features), F32)],
            input_output_aliases={4 + n: n for n in range(len(earlier))},
            compiler_params=params(1),
            cost_estimate=cost(total * features * 1000, total * features * 6),
            name="m_last",
        )(side, value, w_merge, gain_m, *earlier)

    def finish_qkv(side, value, earlier=()):
        return pl.pallas_call(
            qkv_last_kernel,
            grid_spec=pltpu.PrefetchScalarGridSpec(
                num_scalar_prefetch=1,
                grid=(1,),
                in_specs=[pl.BlockSpec((3 * tile, features), lambda i, k: (0, 0)),
                          pl.BlockSpec((tile, 3 * features), lambda i, k: (k[0], 0)),
                          pl.BlockSpec((1, tile), lambda i, k: (0, k[0]))]
                + [pl.BlockSpec(memory_space=pl.ANY)] * len(earlier),
                out_specs=[pl.BlockSpec((tile, 3 * features), lambda i, k: (k[0], 0)),
                           pl.BlockSpec((1, tile), lambda i, k: (0, k[0]))],
            ),
            out_shape=[jax.ShapeDtypeStruct((features, 3 * features), F32),
                       jax.ShapeDtypeStruct((1, features), F32)],
            input_output_aliases={4 + n: n for n in range(len(earlier))},
            compiler_params=params(1),
            cost_estimate=cost(total * features * 500, total * features * 3),
            name="q_last",
        )(side, value, w_qkv, gain_a, *earlier)

    grad_w_merge, grad_w_out, grad_gain_merge = finish_merge(
        theirs, m_got, finish_merge(mine, m_own))
    grad_w_qkv, grad_gain_attn = finish_qkv(theirs, q_got, finish_qkv(mine, q_own))
    grad_gain_merge = grad_gain_merge.reshape(-1)
    grad_gain_attn = grad_gain_attn.reshape(-1)
    return (merged, grad_tokens, grad_gain_attn, grad_w_qkv, grad_w_out, grad_gain_merge,
            grad_w_merge)


def solution(mesh):
    return jax.shard_map(
        on_device_body,
        mesh=mesh,
        in_specs=(P("lat", "lon", None), P(), P(), P(), P(), P(), P(), P("lat", "lon", None)),
        out_specs=(P("lat", "lon", None), P("lat", "lon", None), P(), P(), P(), P(), P()),
        check_vma=False,
    )
```

```python
import functools

import jax
import jax.numpy as jnp
import numpy as np
from jax import lax
from jax.experimental import pallas as pl
from jax.experimental.pallas import tpu as pltpu
from jax.sharding import PartitionSpec as P


WLAT = 6
WLON = 12
EPSILON = 1e-05
EDGE = 8
BF = jnp.bfloat16
F32 = jnp.float32

CALLS = 4


def dot_nn(a, b):
    return lax.dot_general(a, b, (((1,), (0,)), ((), ())), preferred_element_type=F32)


def dot_nt(a, b):
    return lax.dot_general(a, b, (((1,), (1,)), ((), ())), preferred_element_type=F32)


def dot_tn(a, b):
    return lax.dot_general(a, b, (((0,), (0,)), ((), ())), preferred_element_type=F32)


def params(steps):
    return pltpu.CompilerParams(
        dimension_semantics=("arbitrary",) * steps, vmem_limit_bytes=60 * 1024 * 1024
    )


def cost(flops, nbytes):
    return pl.CostEstimate(flops=int(flops), transcendentals=0, bytes_accessed=int(nbytes))


def patch_matrix(cols):
    half = cols // 2
    mat = np.zeros((4 * half, 2 * cols), np.float32)
    for j in range(half):
        for g, (dr, dc) in enumerate(((0, 0), (1, 0), (0, 1), (1, 1))):
            mat[g * half + j, dr * cols + 2 * j + dc] = 1.0
    return mat


def lane_masks():
    lane = lax.broadcasted_iota(jnp.int32, (1, 128), 1)
    even = (lane < 64).astype(F32)
    return even.astype(BF), (1.0 - even).astype(BF)


def load_rows(deep, own_ref, west_ref, south_ref, corner_ref, buf_ref, win_ref, stride):
    tall, wide = win_ref.shape[0] // deep, buf_ref.shape[0] // deep
    for k in range(deep):
        load_windows(pl.program_id(0) * deep + k, k == 0, own_ref, west_ref, south_ref, corner_ref,
                     buf_ref.at[pl.ds(k * wide, wide)], win_ref.at[pl.ds(k * tall, tall)], stride)


def load_windows(step, first, own_ref, west_ref, south_ref, corner_ref, buf_ref, win_ref, stride):
    cols = south_ref.shape[0] // (WLAT // 2)
    wide = EDGE + cols
    half = WLAT // 2

    def put(r, edge, line):
        buf_ref[pl.ds(wide * r, EDGE), :] = edge.astype(F32)
        buf_ref[pl.ds(wide * r + EDGE, cols), :] = line.astype(F32)

    def later(r):
        row = WLAT * step - half + r
        put(r, west_ref[row], own_ref[pl.ds(pl.multiple_of(cols * row, 16), cols), :])

    if first:
        @pl.when(step == 0)
        def _():
            for r in range(half):
                put(r, corner_ref[r], south_ref[pl.ds(cols * r, cols), :])

        @pl.when(step > 0)
        def _():
            for r in range(half):
                later(r)

    for r in range(0 if not first else half, WLAT):
        later(r)
    for b in range(cols // WLON):
        for r in range(WLAT):
            piece = buf_ref[pl.ds(wide * r + EDGE - WLON // 2 + WLON * b, WLON), :]
            win_ref[pl.ds(stride * b + WLON * r, WLON), :] = piece
        pad = stride - WLAT * WLON
        win_ref[pl.ds(stride * (b + 1) - pad, pad), :] = jnp.zeros((pad, win_ref.shape[1]), F32)


def unload_rows(deep, win_ref, grid_ref, stride, out_ref, lon_ref, lat_ref, corner_ref):
    tall, block = win_ref.shape[0] // deep, grid_ref.shape[0] // deep
    cols = block // WLAT
    for k in range(deep):
        for b in range(cols // WLON):
            for r in range(WLAT):
                piece = win_ref[pl.ds(k * tall + stride * b + WLON * r, WLON), :]
                grid_ref[pl.ds(k * block + cols * r + WLON * b, WLON), :] = piece
    out_ref[...] = grid_ref[...].astype(out_ref.dtype)
    edge = [grid_ref[pl.ds(r * cols, EDGE), :] for r in range(deep * WLAT)]
    edge = jnp.concatenate(edge, axis=0).astype(BF)
    lon_ref[...] = edge

    @pl.when(pl.program_id(0) == 0)
    def _():
        lat_ref[...] = grid_ref[pl.ds(0, lat_ref.shape[0]), :].astype(BF)
        corner_ref[...] = edge[: corner_ref.shape[0]]


def stack_heads(value, masks):
    return jnp.concatenate([value * masks[0], value * masks[1]], axis=0)


def forward_kernel(deep, stride, count_b, own_ref, west_ref, south_ref, corner_ref, allow_ref, gain_ref,
                   w_ref, att_ref, qkv_ref, normed_ref, tok_ref, prob_ref, lon_ref, lat_ref,
                   corner_out_ref, buf_ref, win_ref, grid_ref):
    features = own_ref.shape[1]
    load_rows(deep, own_ref, west_ref, south_ref, corner_ref, buf_ref, win_ref, stride)
    x = win_ref[...]
    tok_ref[...] = x.astype(BF)
    average = jnp.mean(x, axis=-1, keepdims=True)
    centered = x - average
    variance = jnp.mean(centered * centered, axis=-1, keepdims=True)
    normed = (centered * lax.rsqrt(variance + EPSILON) * gain_ref[...]).astype(BF)
    normed_ref[...] = normed
    for t in range(3):
        qkv_ref[t] = dot_nn(normed, w_ref[:, features * t : features * (t + 1)]).astype(BF)
    masks = lane_masks()
    for b in range(deep * count_b):
        allow = allow_ref[b // count_b] > 0.5
        rows = slice(b * stride, (b + 1) * stride)
        for pair in range(features // 128):
            lanes = pl.ds(128 * pair, 128)
            q2 = qkv_ref[0, rows, lanes] * jnp.asarray(0.125, BF)
            s2 = dot_nt(stack_heads(qkv_ref[1, rows, lanes], masks), q2)
            probs = []
            for h in range(2):
                s = jnp.where(allow, s2[h * stride : (h + 1) * stride], -1e30)
                e = jnp.exp(s - jnp.max(s, axis=0, keepdims=True))
                probs.append((e * (1.0 / jnp.sum(e, axis=0, keepdims=True))).astype(BF))
            p2 = jnp.concatenate(probs, axis=0)
            prob_ref[pair, pl.ds(2 * stride * b, 2 * stride), :] = p2
            win_ref[rows, lanes] = dot_tn(p2, stack_heads(qkv_ref[2, rows, lanes], masks))
    unload_rows(deep, win_ref, grid_ref, stride, att_ref, lon_ref, lat_ref, corner_out_ref)


def assemble_kernel(deep, stride, own_ref, west_ref, south_ref, corner_ref, out_ref, buf_ref, win_ref):
    load_rows(deep, own_ref, west_ref, south_ref, corner_ref, buf_ref, win_ref, stride)
    out_ref[...] = win_ref[...].astype(BF)


def middle_kernel(cols, tok_ref, att_ref, w_out_ref, gain_ref, grad_in_ref, to_patch_ref,
                  from_patch_ref, merged_in_ref, grad_mixed_ref, grad_att_ref, lon_ref, lat_ref,
                  corner_ref):
    tokens, features = tok_ref.shape
    pairs = tokens // (2 * cols)
    half = cols // 2
    mixed = (tok_ref[...].astype(F32) + dot_nn(att_ref[...], w_out_ref[...])).astype(BF)
    parts = [dot_nn(to_patch_ref[...], mixed[2 * cols * i : 2 * cols * (i + 1)]) for i in range(pairs)]
    groups = [
        jnp.concatenate([part[half * g : half * (g + 1)] for part in parts], axis=0) for g in range(4)
    ]
    width = 4 * features
    average = sum(jnp.sum(v, axis=-1, keepdims=True) for v in groups) / width
    groups = [v - average for v in groups]
    variance = sum(jnp.sum(v * v, axis=-1, keepdims=True) for v in groups) / width
    inv = lax.rsqrt(variance + EPSILON)
    groups = [v * inv for v in groups]
    grads = []
    for g in range(4):
        span = slice(features * g, features * (g + 1))
        gain = gain_ref[:, span]
        merged_in_ref[:, span] = (groups[g] * gain).astype(BF)
        grads.append(grad_in_ref[:, span].astype(F32) * gain)
    mean_one = sum(jnp.sum(v, axis=-1, keepdims=True) for v in grads) / width
    mean_two = sum(
        jnp.sum(v * h, axis=-1, keepdims=True) for v, h in zip(grads, groups)
    ) / width
    outs = [(v - mean_one - h * mean_two) * inv for v, h in zip(grads, groups)]
    for i in range(pairs):
        piece = jnp.concatenate([v[half * i : half * (i + 1)] for v in outs], axis=0).astype(BF)
        back = dot_nn(from_patch_ref[...], piece).astype(BF)
        grad_mixed_ref[pl.ds(2 * cols * i, 2 * cols), :] = back
    grad_att = dot_nt(grad_mixed_ref[...], w_out_ref[...])
    grad_att_ref[...] = grad_att.astype(BF)
    edge = [grad_att[r * cols - EDGE : r * cols] for r in range(1, tokens // cols + 1)]
    lon_ref[...] = jnp.concatenate(edge, axis=0).astype(BF)

    @pl.when(pl.program_id(0) == pl.num_programs(0) - 1)
    def _():
        lat_ref[...] = grad_att[tokens - lat_ref.shape[0] :].astype(BF)
        corner_ref[...] = jnp.concatenate(edge[-(WLAT // 2) :], axis=0).astype(BF)


def grad_in_kernel(gm_ref, w_merge_ref, out_ref):
    out_ref[...] = dot_nt(gm_ref[...], w_merge_ref[...]).astype(BF)


def merge_grad_kernel(_, merged_in_ref, gm_ref, out_ref):
    out_ref[...] = dot_tn(merged_in_ref[...], gm_ref[...]).astype(BF)


def row_sums(value):
    total = sum(value[:, 128 * k : 128 * (k + 1)] for k in range(value.shape[1] // 128))
    return jnp.sum(total.T, axis=0, keepdims=True)


def merge_last_kernel(_, value_ref, w_ref, gain_ref, *refs):
    out_ref, dgain_ref = refs[-2:]
    value = value_ref[...].astype(F32)
    out_ref[...] = value
    dgain_ref[...] = row_sums(value * w_ref[...].astype(F32)) / gain_ref[...]


def qkv_last_kernel(_, value_ref, w_ref, gain_ref, *refs):
    out_ref, out_o_ref, dgain_ref = refs[-3:]
    height, features = value_ref.shape[0] // 4, value_ref.shape[1]
    out_o_ref[...] = value_ref[3 * height :, :].astype(F32)
    total = 0.0
    for t in range(3):
        lanes = slice(features * t, features * (t + 1))
        value = value_ref[height * t : height * (t + 1), :].astype(F32)
        out_ref[:, lanes] = value
        total = total + value * w_ref[:, lanes].astype(F32)
    dgain_ref[...] = row_sums(total) / gain_ref[...]


def backward_kernel(stride, count_b, ga_ref, qkv_ref, prob_ref, prev_ref, gqkv_ref):
    del prev_ref
    masks = lane_masks()
    low = lax.broadcasted_iota(jnp.int32, (1, 128), 1) < 64
    spans = [slice(b * stride, (b + 1) * stride) for b in range(count_b)]
    for pair in range(ga_ref.shape[1] // 128):
        lanes = pl.ds(128 * pair, 128)
        work = []
        for b, rows in enumerate(spans):
            do2 = ga_ref[rows, lanes]
            p2 = prob_ref[pair, pl.ds(2 * stride * b, 2 * stride), :]
            dp2 = dot_nt(stack_heads(qkv_ref[2, rows, lanes], masks), do2)
            dv = dot_nn(p2, do2)
            gqkv_ref[2, rows, lanes] = jnp.where(low, dv[:stride], dv[stride:]).astype(BF)
            work.append((p2, dp2))
        scores = []
        for p2, dp2 in work:
            grads = []
            for h in range(2):
                p = p2[h * stride : (h + 1) * stride].astype(F32)
                dp = dp2[h * stride : (h + 1) * stride]
                grads.append((p * (dp - jnp.sum(dp * p, axis=0, keepdims=True))).astype(BF))
            scores.append(jnp.concatenate(grads, axis=0))
        for rows, ds2 in zip(spans, scores):
            q2 = qkv_ref[0, rows, lanes] * jnp.asarray(0.125, BF)
            dk = dot_nn(ds2, q2)
            dq = dot_tn(ds2, stack_heads(qkv_ref[1, rows, lanes], masks))
            gqkv_ref[0, rows, lanes] = (dq * 0.125).astype(BF)
            gqkv_ref[1, rows, lanes] = jnp.where(low, dk[:stride], dk[stride:]).astype(BF)


def qkv_grad_kernel(_, normed_ref, gqkv_ref, att_ref, gmix_ref, out_ref):
    height = normed_ref.shape[1]
    for t in range(3):
        out_ref[height * t : height * (t + 1), :] = dot_tn(normed_ref[...], gqkv_ref[t]).astype(BF)
    out_ref[3 * height :, :] = dot_tn(att_ref[...], gmix_ref[...]).astype(BF)


def input_grad_kernel(deep, stride, gqkv_ref, x_ref, gain_ref, w_ref, out_ref, lon_ref, lat_ref, corner_ref,
                      win_ref, grid_ref):
    features = x_ref.shape[1]
    grad = sum(dot_nt(gqkv_ref[t], w_ref[:, features * t : features * (t + 1)]) for t in range(3))
    x = x_ref[...].astype(F32)
    centered = x - jnp.mean(x, axis=-1, keepdims=True)
    inv = lax.rsqrt(jnp.mean(centered * centered, axis=-1, keepdims=True) + EPSILON)
    hat = centered * inv
    grad = grad * gain_ref[...]
    one = jnp.mean(grad, axis=-1, keepdims=True)
    two = jnp.mean(grad * hat, axis=-1, keepdims=True)
    win_ref[...] = (grad - one - hat * two) * inv
    unload_rows(deep, win_ref, grid_ref, stride, out_ref, lon_ref, lat_ref, corner_ref)


def merged_kernel(a_ref, w_ref, out_ref):
    out_ref[...] = dot_nn(a_ref[...], w_ref[...]).astype(BF)


def whole(shape):
    return pl.BlockSpec(shape, lambda i: (0,) * len(shape))


def rows_of(height, width):
    return pl.BlockSpec((height, width), lambda i: (i, 0))


def shift_pairs(count_lat, count_lon, dlat, dlon):
    return [
        (a * count_lon + b, ((a + dlat) % count_lat) * count_lon + (b + dlon) % count_lon)
        for a in range(count_lat)
        for b in range(count_lon)
    ]


def send(value, dlat, dlon):
    pairs = shift_pairs(lax.axis_size("lat"), lax.axis_size("lon"), dlat, dlon)
    return lax.ppermute(value, ("lat", "lon"), pairs)


def exchange(parts, sign):
    lon_edge, lat_edge, corner = parts
    lon_edge = send(lon_edge, 0, sign)
    lat_edge = send(lat_edge, sign, 0)
    corner = send(corner, sign, sign)
    return lon_edge, lat_edge, corner


def edges(values):
    rows, cols, features = values.shape
    hr = WLAT // 2
    parts = (values[:, cols - EDGE :], values[rows - hr :], values[rows - hr :, cols - EDGE :])
    return [v.reshape(-1, features) for v in parts]


def to_own(values, parts):
    rows, cols, features = values.shape
    hr, hc = WLAT // 2, WLON // 2
    east, north, corner = (v.astype(values.dtype) for v in parts)
    top = jnp.concatenate([values[hr:, hc:], east.reshape(rows, EDGE, features)[hr:, :hc]], axis=1)
    north = north.reshape(hr, cols, features)[:, hc:]
    bottom = jnp.concatenate([north, corner.reshape(hr, EDGE, features)[:, :hc]], axis=1)
    return jnp.concatenate([top, bottom], axis=0)


def part_sum(terms, index, height):
    parts = [lax.dynamic_slice_in_dim(t, index * height, height, 0).astype(F32) for t in terms]
    return sum(parts[1:], parts[0]).astype(BF)


def join(value, received, keep):
    first = jnp.where(keep == 0, value, received)
    second = jnp.where(keep == 0, received, value)
    return jnp.concatenate([first, second], axis=0)


def reduce_all(sent, kept):
    count_lat, count_lon = lax.axis_size("lat"), lax.axis_size("lon")
    bits = count_lon.bit_length() - 1
    me, lat = lax.axis_index("lon"), lax.axis_index("lat")
    odd = lax.rem(me, 2)
    partner = [(i, i ^ 1) for i in range(count_lon)]
    plans = []
    for k in range(bits - 1):
        low, high = 2 << k, 2 << (bits - 2 - k)
        pairs = [(i, i ^ (low if i % 2 == 0 else high)) for i in range(count_lon)]
        keep = jnp.where(odd == 0, lax.rem(me // low, 2), lax.rem(me // high, 2))
        plans.append((pairs, keep))
    received = lax.ppermute(sent, "lon", partner)
    terms, height = [kept, received], kept.shape[0]
    for k, (pairs, keep) in enumerate(plans, 1):
        height = height // 2
        sent = part_sum(terms, 1 - keep, height)
        received = lax.ppermute(sent, "lon", pairs)
        terms = [lax.dynamic_slice_in_dim(t, keep * height, height, 0) for t in terms] + [received]
    height = height // count_lat
    total = [lax.dynamic_slice_in_dim(t, lat * height, height, 0).astype(F32) for t in terms]
    for d in range(1, count_lat):
        sent = part_sum(terms, lat ^ d, height)
        received = lax.ppermute(sent, "lat", [(i, i ^ d) for i in range(count_lat)])
        total.append(received.astype(F32))
    mine = sum(total[1:], total[0]).astype(BF)
    value = jnp.zeros((count_lat * height,) + mine.shape[1:], BF)
    value = lax.dynamic_update_slice_in_dim(value, mine, lat * height, 0)
    for d in range(1, count_lat):
        received = lax.ppermute(mine, "lat", [(i, i ^ d) for i in range(count_lat)])
        value = lax.dynamic_update_slice_in_dim(value, received, (lat ^ d) * height, 0)
    for k, (pairs, keep) in reversed(list(enumerate(plans, 1))):
        received = lax.ppermute(value, "lon", pairs)
        value = join(value, received, keep)
    received = lax.ppermute(value, "lon", partner)
    return value, received


def on_device_body(tokens, lat_band, gain_attn, w_qkv, w_out, gain_merge, w_merge, grad_merged):
    rows, cols, features = tokens.shape
    width2 = grad_merged.shape[2]
    count_a, count_b = rows // WLAT, cols // WLON
    window = WLAT * WLON
    stride = -(-window // 16) * 16
    half_lat = WLAT // 2
    block = WLAT * cols
    wide = WLAT * (cols + EDGE)
    padded = count_b * stride
    total = rows * cols
    patch_np = patch_matrix(cols)
    to_patch = jnp.asarray(patch_np, BF)
    from_patch = jnp.asarray(patch_np.T, BF)

    band_count = lat_band.shape[0]
    extended = jnp.concatenate([lat_band[band_count - half_lat :], lat_band])
    band_rows = lax.dynamic_slice_in_dim(extended, lax.axis_index("lat") * rows, rows)
    labels = jnp.repeat(band_rows.reshape(count_a, WLAT), WLON, axis=1)
    labels = jnp.pad(labels, ((0, 0), (0, stride - window)), constant_values=-1)
    allow = (labels[:, :, None] == labels[:, None, :]).astype(F32)
    gain_a = gain_attn.reshape(1, features)
    gain_m = gain_merge.reshape(1, 4 * features)

    own_tok = tokens.reshape(total, features)
    edge_shapes = [(rows * EDGE, features), (half_lat * cols, features), (half_lat * EDGE, features)]
    edge_types = [jax.ShapeDtypeStruct(shape, BF) for shape in edge_shapes]
    deep = 2 if count_a % 2 == 0 else 1
    edge_specs = [rows_of(deep * WLAT * EDGE, features), whole(edge_shapes[1]), whole(edge_shapes[2])]
    halo_specs = [whole((total, features)), whole((rows, EDGE, features)), whole(edge_shapes[1]),
                  whole((half_lat, EDGE, features))]
    win_scratch = pltpu.VMEM((deep * padded, features), F32)
    buf_scratch = pltpu.VMEM((deep * wide, features), F32)
    grid_scratch = pltpu.VMEM((deep * block, features), F32)

    def halo_args(parts):
        west, south, corner = parts
        return west.reshape(rows, EDGE, features), south, corner.reshape(half_lat, EDGE, features)

    tok_halos = exchange(edges(tokens), 1)
    allow_spec = pl.BlockSpec((deep, stride, stride), lambda i: (i, 0, 0))
    pairs = features // 128
    tall3 = count_a * padded
    qkv_spec = pl.BlockSpec((3, deep * padded, features), lambda i: (0, i, 0))
    prob_rows = 2 * stride * count_b
    attended, qkv, normed, tok_win, probs, *att_edges = pl.pallas_call(
        functools.partial(forward_kernel, deep, stride, count_b),
        grid=(count_a // deep,),
        in_specs=halo_specs + [allow_spec, whole((1, features)), whole((features, 3 * features))],
        out_specs=[rows_of(deep * block, features), qkv_spec, rows_of(deep * padded, features),
                   rows_of(deep * padded, features),
                   pl.BlockSpec((pairs, deep * prob_rows, stride), lambda i: (0, i, 0))] + edge_specs,
        out_shape=[jax.ShapeDtypeStruct((total, features), BF),
                   jax.ShapeDtypeStruct((3, tall3, features), BF),
                   jax.ShapeDtypeStruct((tall3, features), BF),
                   jax.ShapeDtypeStruct((tall3, features), BF),
                   jax.ShapeDtypeStruct((pairs, count_a * prob_rows, stride), BF)] + edge_types,
        scratch_shapes=[buf_scratch, win_scratch, grid_scratch],
        compiler_params=params(1),
        cost_estimate=cost(4 * total * features * 3 * features, 2 * total * features * 8),
        name="attn_fwd",
    )(own_tok, *halo_args(tok_halos), allow, gain_a, w_qkv)

    att_parts = exchange(att_edges, -1)
    own_att = to_own(attended.reshape(rows, cols, features), att_parts).reshape(total, features)
    gm = grad_merged.reshape(total // 4, width2)
    grad_in = pl.pallas_call(
        grad_in_kernel,
        grid=(2,),
        in_specs=[whole((total // 4, width2)), rows_of(2 * features, width2)],
        out_specs=pl.BlockSpec((total // 4, 2 * features), lambda i: (0, i)),
        out_shape=jax.ShapeDtypeStruct((total // 4, 4 * features), BF),
        compiler_params=params(1),
        cost_estimate=cost(2 * total * features * width2, 2 * total * features * 4),
        name="grad_in",
    )(gm, w_merge)

    steps = 2
    tall = total // steps
    short = tall // 4
    merged_in, grad_mixed, grad_att, *grad_edges = pl.pallas_call(
        functools.partial(middle_kernel, cols),
        grid=(steps,),
        in_specs=[rows_of(tall, features), rows_of(tall, features), whole((features, features)),
                  whole((1, 4 * features)), rows_of(short, 4 * features),
                  whole((2 * cols, 2 * cols)), whole((2 * cols, 2 * cols))],
        out_specs=[rows_of(short, 4 * features), rows_of(tall, features), rows_of(tall, features),
                   rows_of(edge_shapes[0][0] // steps, features)] + edge_specs[1:],
        out_shape=[jax.ShapeDtypeStruct((total // 4, 4 * features), BF),
                   jax.ShapeDtypeStruct((total, features), BF),
                   jax.ShapeDtypeStruct((total, features), BF)] + edge_types,
        compiler_params=params(1),
        cost_estimate=cost(8 * total * features * features, 2 * total * features * 6),
        name="merge_mid",
    )(own_tok, own_att, w_out, gain_m, grad_in, to_patch, from_patch)

    att_halos = exchange(grad_edges, 1)
    pieces = 4
    odd = lax.rem(lax.axis_index("lon"), 2).astype(jnp.int32)
    mine, theirs = odd.reshape(1), (1 - odd).reshape(1)

    def merge_dw(side):
        return pl.pallas_call(
            merge_grad_kernel,
            grid_spec=pltpu.PrefetchScalarGridSpec(
                num_scalar_prefetch=1,
                grid=(pieces // 2,),
                in_specs=[pl.BlockSpec((total // 4, features), lambda i, k: (0, 2 * k[0] + i)),
                          pl.BlockSpec((total // 4, width2), lambda i, k: (0, 0))],
                out_specs=pl.BlockSpec((features, width2), lambda i, k: (i, 0)),
            ),
            out_shape=jax.ShapeDtypeStruct((pieces // 2 * features, width2), BF),
            compiler_params=params(1),
            cost_estimate=cost(2 * total * features * features * 2, total * features * 6),
            name="merge_dw",
        )(side, merged_in, gm)

    m_own, m_got = reduce_all(merge_dw(theirs), merge_dw(mine))

    grad_win = pl.pallas_call(
        functools.partial(assemble_kernel, count_a, stride),
        grid=(1,),
        in_specs=halo_specs,
        out_specs=rows_of(tall3, features),
        out_shape=jax.ShapeDtypeStruct((tall3, features), BF),
        scratch_shapes=[pltpu.VMEM((count_a * wide, features), F32), pltpu.VMEM((tall3, features), F32)],
        compiler_params=params(1),
        cost_estimate=cost(total * features * 1200, 2 * total * features * 3),
        name="assemble",
    )(grad_att, *halo_args(att_halos))
    calls = CALLS
    lane_count = features // calls
    grad_qkv = None
    for j in range(calls):
        spec = pl.BlockSpec((3, deep * padded, lane_count), lambda i, j=j: (0, i, j))
        operands = [grad_win, qkv, probs]
        specs = [pl.BlockSpec((deep * padded, lane_count), lambda i, j=j: (i, j)), spec,
                 pl.BlockSpec((pairs // calls, deep * prob_rows, stride), lambda i, j=j: (j, i, 0))]
        if grad_qkv is not None:
            operands.append(grad_qkv)
            specs.append(pl.BlockSpec(memory_space=pl.ANY))
            body = functools.partial(backward_kernel, stride, deep * count_b)
        else:
            def body(ga_ref, qkv_ref, prob_ref, gqkv_ref):
                backward_kernel(stride, deep * count_b, ga_ref, qkv_ref, prob_ref, None, gqkv_ref)
        grad_qkv = pl.pallas_call(
            body,
            grid=(count_a // deep,),
            in_specs=specs,
            out_specs=spec,
            out_shape=jax.ShapeDtypeStruct((3, tall3, features), BF),
            input_output_aliases={3: 0} if j else {},
            compiler_params=params(1),
            cost_estimate=cost(4 * total * features * 3 * features // calls,
                               2 * total * features * 8 // calls),
        )(*operands)
    tile = features // 2

    def qkv_dw(side):
        return pl.pallas_call(
            qkv_grad_kernel,
            grid_spec=pltpu.PrefetchScalarGridSpec(
                num_scalar_prefetch=1,
                grid=(1,),
                in_specs=[pl.BlockSpec((tall3, tile), lambda i, k: (0, k[0])),
                          pl.BlockSpec((3, tall3, features), lambda i, k: (0, 0, 0)),
                          pl.BlockSpec((total, tile), lambda i, k: (0, k[0])),
                          pl.BlockSpec((total, features), lambda i, k: (0, 0))],
                out_specs=pl.BlockSpec((4 * tile, features), lambda i, k: (0, 0)),
            ),
            out_shape=jax.ShapeDtypeStruct((4 * tile, features), BF),
            compiler_params=params(1),
            cost_estimate=cost(total * features * 3 * features, total * features * 5),
            name="qkv_dw",
        )(side, normed, grad_qkv, own_att, grad_mixed)

    q_own, q_got = reduce_all(qkv_dw(theirs), qkv_dw(mine))

    grad_inputs, *in_edges = pl.pallas_call(
        functools.partial(input_grad_kernel, deep, stride),
        grid=(count_a // deep,),
        in_specs=[qkv_spec, rows_of(deep * padded, features), whole((1, features)),
                  whole((features, 3 * features))],
        out_specs=[rows_of(deep * block, features)] + edge_specs,
        out_shape=[jax.ShapeDtypeStruct((total, features), BF)] + edge_types,
        scratch_shapes=[win_scratch, grid_scratch],
        compiler_params=params(1),
        cost_estimate=cost(2 * total * features * 3 * features, 2 * total * features * 6),
        name="input_grad",
    )(grad_qkv, tok_win, gain_a, w_qkv)
    in_parts = exchange(in_edges, -1)
    grad_own = to_own(grad_inputs.reshape(rows, cols, features), in_parts)
    grad_tokens = grad_own.astype(F32) + grad_mixed.reshape(rows, cols, features).astype(F32)

    merged = pl.pallas_call(
        merged_kernel,
        grid=(2,),
        in_specs=[whole((total // 4, 4 * features)),
                  pl.BlockSpec((4 * features, width2 // 2), lambda i: (0, i))],
        out_specs=pl.BlockSpec((total // 4, width2 // 2), lambda i: (0, i)),
        out_shape=jax.ShapeDtypeStruct((total // 4, width2), BF),
        compiler_params=params(1),
        cost_estimate=cost(2 * total * features * width2, 2 * total * features * 4),
        name="merged",
    )(merged_in, w_merge).reshape(grad_merged.shape)

    def finish_merge(side, value, earlier=()):
        return pl.pallas_call(
            merge_last_kernel,
            grid_spec=pltpu.PrefetchScalarGridSpec(
                num_scalar_prefetch=1,
                grid=(pieces // 2,),
                in_specs=[pl.BlockSpec((features, width2), lambda i, k: (i, 0)),
                          pl.BlockSpec((features, width2), lambda i, k: (2 * k[0] + i, 0)),
                          pl.BlockSpec((1, features), lambda i, k: (0, 2 * k[0] + i))]
                + [pl.BlockSpec(memory_space=pl.ANY)] * len(earlier),
                out_specs=[pl.BlockSpec((features, width2), lambda i, k: (2 * k[0] + i, 0)),
                           pl.BlockSpec((1, features), lambda i, k: (0, 2 * k[0] + i))],
            ),
            out_shape=[jax.ShapeDtypeStruct((pieces * features, width2), F32),
                       jax.ShapeDtypeStruct((1, pieces * features), F32)],
            input_output_aliases={4 + n: n for n in range(len(earlier))},
            compiler_params=params(1),
            cost_estimate=cost(total * features * 1000, total * features * 6),
            name="m_last",
        )(side, value, w_merge, gain_m, *earlier)

    def finish_qkv(side, value, earlier=()):
        return pl.pallas_call(
            qkv_last_kernel,
            grid_spec=pltpu.PrefetchScalarGridSpec(
                num_scalar_prefetch=1,
                grid=(1,),
                in_specs=[pl.BlockSpec((4 * tile, features), lambda i, k: (0, 0)),
                          pl.BlockSpec((tile, 3 * features), lambda i, k: (k[0], 0)),
                          pl.BlockSpec((1, tile), lambda i, k: (0, k[0]))]
                + [pl.BlockSpec(memory_space=pl.ANY)] * len(earlier),
                out_specs=[pl.BlockSpec((tile, 3 * features), lambda i, k: (k[0], 0)),
                           pl.BlockSpec((tile, features), lambda i, k: (k[0], 0)),
                           pl.BlockSpec((1, tile), lambda i, k: (0, k[0]))],
            ),
            out_shape=[jax.ShapeDtypeStruct((features, 3 * features), F32),
                       jax.ShapeDtypeStruct((features, features), F32),
                       jax.ShapeDtypeStruct((1, features), F32)],
            input_output_aliases={4 + n: n for n in range(len(earlier))},
            compiler_params=params(1),
            cost_estimate=cost(total * features * 500, total * features * 3),
            name="q_last",
        )(side, value, w_qkv, gain_a, *earlier)

    grad_w_merge, grad_gain_merge = finish_merge(
        theirs, m_got, finish_merge(mine, m_own))
    grad_w_qkv, grad_w_out, grad_gain_attn = finish_qkv(
        theirs, q_got, finish_qkv(mine, q_own))
    grad_gain_merge = grad_gain_merge.reshape(-1)
    grad_gain_attn = grad_gain_attn.reshape(-1)
    return (merged, grad_tokens, grad_gain_attn, grad_w_qkv, grad_w_out, grad_gain_merge,
            grad_w_merge)


def solution(mesh):
    return jax.shard_map(
        on_device_body,
        mesh=mesh,
        in_specs=(P("lat", "lon", None), P(), P(), P(), P(), P(), P(), P("lat", "lon", None)),
        out_specs=(P("lat", "lon", None), P("lat", "lon", None), P(), P(), P(), P(), P()),
        check_vma=False,
    )
```
